32 devices in a mesh: seq: 32 (over z, y, x, core).
Axes of the slice: x: 2, y: 2, z: 4, core: 2. Of those that a mesh axis runs over, the one named last changes fastest.
Arguments:
- history: float32 [12288, 1024], P('seq'), may hold values from -6 to 6
- taps: float32 [12288, 1024], P('seq'), may hold values from -0.109375 to 0.109375
- self_taps: float32 [1024, 256], P('seq'), may hold values from -0.375 to 0.375
- fresh: float32 [1024, 256], P('seq'), may hold values from -6 to 6
- gate: float32 [1024, 256], P('seq'), may hold values from -6 to 6
Outputs:
- gated: float32 [1024, 256], P('seq')
The draws below stay inside these ranges and needn't reach their ends.
All inputs are finite; a program needn't handle non-finite values.
Results may differ from the reference program's by a relative error of at most 0.000053.
Values sent between devices are 32-bit elements; how exact they have to be, the bound alone decides.
A program may use at most 64 MiB of HBM per device.

```python
import jax
import jax.numpy as jnp
from jax import lax

CHANNELS = 1024
NEW_TOKENS = 256
HISTORY = 12288


def raised(entries, key, source, target, shards_of, factor):
    owner, partner = [(jnp.arange(entries.shape[dim]) // (entries.shape[dim] // shards_of)).reshape([-1 if axis == dim else 1 for axis in range(entries.ndim)]) for dim in (source, target)]
    chosen = jax.random.permutation(key, shards_of)[partner]
    strong = (owner == chosen) | (owner == (partner + shards_of // 2) % shards_of)
    return jnp.where(strong, factor * entries, entries)


def steps_of(own_key, shape, shards, smallest, high):
    gain, own = 1.0, jax.random.fold_in(own_key, 6)
    for dim, shards_of in shards:
        heights = jnp.exp(jax.random.uniform(jax.random.fold_in(own, dim), (shards_of,), jnp.float32, smallest / len(shards), high / len(shards)))
        gain = gain * jnp.repeat(heights, shape[dim] // shards_of).reshape([-1 if axis == dim else 1 for axis in range(len(shape))])
    return gain


def gaussian(rng, shape, deviation, reach, split=(), dtype=jnp.bfloat16):
    level = steps_of(rng, shape, split, -0.22, 0.18) if split else 1.0
    entries = jax.random.normal(rng, shape, jnp.float32) * deviation * level
    return jnp.minimum(jnp.maximum(entries, -reach), reach).astype(dtype)


def heavy_noise(own_key, shape, spread, most, split, heavy, held_as=jnp.bfloat16):
    array = spread * jax.random.normal(own_key, shape, jnp.float32)
    if split:
        array = array * steps_of(own_key, shape, split, -0.22, 0.18)
    return jnp.clip(raised(array, jax.random.fold_in(own_key, 3), *heavy), -most, most).astype(held_as)


def setup_inputs(seed: int = 0) -> dict:
    arg_keys = jax.random.split(jax.random.key(seed), 6)
    return {
        "history": gaussian(arg_keys[0], (HISTORY, CHANNELS), 1.0, 6.0, ((0, 32),), jnp.float32),
        "taps": heavy_noise(arg_keys[1], (HISTORY, CHANNELS), HISTORY ** -0.5, 0.109375, ((0, 32),), (0, 1, 32, 2.75), jnp.float32),
        "self_taps": gaussian(arg_keys[2], (CHANNELS, NEW_TOKENS), NEW_TOKENS ** -0.5, 0.375, ((0, 32),), jnp.float32),
        "fresh": gaussian(arg_keys[3], (CHANNELS, NEW_TOKENS), 1.0, 6.0, ((0, 32),), jnp.float32),
        "gate": gaussian(arg_keys[4], (CHANNELS, NEW_TOKENS), 1.0, 6.0, ((0, 32),), jnp.float32),
    }


def correlate(pair):
    hist_block, taps_block = pair
    length = 2 * HISTORY
    hist_spec = jnp.fft.rfft(hist_block, n=length, axis=0)
    taps_spec = jnp.fft.rfft(taps_block, n=length, axis=0)
    return jnp.fft.irfft(jnp.conj(taps_spec) * hist_spec, n=length, axis=0)[:NEW_TOKENS]


def reference(history, taps, self_taps, fresh, gate):
    groups = CHANNELS // 32
    hist_blocks = history.reshape(HISTORY, groups, 32).transpose(1, 0, 2)
    taps_blocks = taps.reshape(HISTORY, groups, 32).transpose(1, 0, 2)
    lagged = lax.map(correlate, (hist_blocks, taps_blocks))
    hist_part = lagged.transpose(0, 2, 1).reshape(CHANNELS, NEW_TOKENS)
    doubled = 2 * NEW_TOKENS
    own_spec = jnp.fft.rfft(self_taps, n=doubled, axis=1) * jnp.fft.rfft(fresh, n=doubled, axis=1)
    own_part = jnp.fft.irfft(own_spec, n=doubled, axis=1)[:, :NEW_TOKENS]
    return gate * (hist_part + own_part)
```

```python
import math

import jax
import jax.numpy as jnp
import numpy as np
from jax import lax
from jax.experimental import pallas as pl
from jax.experimental.pallas import tpu as pltpu
from jax.sharding import PartitionSpec as P

AXIS = "seq"
PLANE = 8
MESH = pl.DeviceIdType.MESH
F32 = jnp.float32
BF16 = jnp.bfloat16


def dft_matrix(seg):
    phase = np.outer(4 * np.arange(seg) + 1, np.arange(seg)) % (4 * seg)
    angle = phase * (math.pi / (2 * seg))
    return np.concatenate([np.cos(angle), -np.sin(angle)], axis=0)


def halves(matrix):
    high = np.asarray(matrix, np.float32).astype(BF16)
    low = np.asarray(matrix - high.astype(np.float64), np.float32).astype(BF16)
    return high, low


def split(value):
    high = value.astype(BF16)
    return high, (value - high.astype(F32)).astype(BF16)


def mul_conj(a, b):
    return a[0] * b[0] + a[1] * b[1], a[1] * b[0] - a[0] * b[1]


def mul(a, b):
    return a[0] * b[0] - a[1] * b[1], a[0] * b[1] + a[1] * b[0]


def add(a, b):
    return a[0] + b[0], a[1] + b[1]


def turn(a):
    return -a[1], a[0]


def back(a):
    return a[1], -a[0]


def local_products(hs, ts):
    us = [None] + [add(ts[a], turn(ts[a - 1])) for a in range(1, len(ts))]
    first = mul_conj(hs[0], ts[0])
    for a in range(1, len(hs)):
        first = add(first, mul_conj(hs[a], us[a]))
    second = mul_conj(hs[1], ts[0])
    for a in range(2, len(hs)):
        second = add(second, mul_conj(hs[a], us[a - 1]))
    return first, second


def halo_products(first, second, h0, h1, t_near, t_before, h_after):
    one = mul_conj(h0, t_before)
    two = add(mul_conj(h1, t_before), mul_conj(h_after, t_near))
    return add(first, back(one)), add(add(second, one), back(two))


def own_products(f0, f1, s0, s1):
    first = mul(f0, s0)
    return first, add(turn(first), add(mul(f0, s1), mul(f1, s0)))


def plain_body(history, taps, self_taps, fresh, gate):
    n = lax.axis_size(AXIS)
    seg = fresh.shape[1] // 2
    matrix = jnp.asarray(dft_matrix(seg).astype(np.float32))
    hp = lax.Precision.HIGHEST
    before = lax.ppermute(taps[-seg:], AXIS, [(s, s + 1) for s in range(n - 1)])
    after = lax.ppermute(history[:seg], AXIS, [(s, s - 1) for s in range(1, n)])

    def forward(rows):
        spec = jnp.dot(matrix, rows, precision=hp)
        return spec[:seg], spec[seg:]

    def inverse(spec):
        return jnp.dot(matrix.T / seg, jnp.concatenate(spec, axis=0), precision=hp)

    count = history.shape[0] // seg
    hs = [forward(history[a * seg : (a + 1) * seg]) for a in range(count)]
    ts = [forward(taps[a * seg : (a + 1) * seg]) for a in range(count)]
    first, second = local_products(hs, ts)
    first, second = halo_products(first, second, hs[0], hs[1], ts[-2], forward(before), forward(after))
    part = jnp.concatenate([inverse(first), inverse(second)], axis=0).T
    summed = lax.psum_scatter(part, AXIS, scatter_dimension=0, tiled=True)
    f, s = fresh.T, self_taps.T
    own = own_products(forward(f[:seg]), forward(f[seg:]), forward(s[:seg]), forward(s[seg:]))
    own_part = jnp.concatenate([inverse(own[0]), inverse(own[1])], axis=0).T
    return gate * (summed + own_part)


def kernel(n, seg, hist, taps, self_taps, fresh, gate, fh, fl, gh, gl, out,
           hist_v, taps_v, tb, ha, sh0, sh1, st1, q0, q1, parts, d_recv, p_send, p_recv, z_send, z_recv,
           load_sem, tb_s, tb_r, ha_s, ha_r, d_s, d_r, p_s, p_r, z_s, z_r):
    me = lax.axis_index(AXIS)
    nz = n // PLANE
    my_z, low = me // PLANE, me % PLANE
    core, spot = me % 2, low // 2
    rows = hist.shape[0]
    count = rows // seg
    width = hist.shape[1] // nz
    block = width // PLANE
    partner = me + 1 - 2 * core
    chips = PLANE // 2

    def lanes(z, i):
        return pl.ds(pl.multiple_of(((z + 1 + i) % nz) * width, width), width)

    def plane_peer(j):
        bit0, bit1 = spot % 2, spot // 2
        other = (bit0 + j % 2) % 2 + 2 * ((bit1 + j // 2) % 2)
        return other, me - low + other * 2 + core

    def remote(src, dst, send, recv, dev):
        return pltpu.make_async_remote_copy(
            src_ref=src, dst_ref=dst, send_sem=send, recv_sem=recv, device_id=(dev,), device_id_type=MESH
        )

    loads = []
    for i in range(nz):
        for k, (src, dst) in enumerate(((hist, hist_v), (taps, taps_v))):
            copy = pltpu.make_async_copy(src.at[:, lanes(my_z, i)], dst.at[i], load_sem.at[k, i])
            copy.start()
            loads.append(copy)

    outer = (me + 2 * core - 1 + n) % n
    peers = [partner, outer]
    peers += [plane_peer(j)[1] for j in range(1, chips)]
    peers += [(me + k * PLANE) % n for k in range(1, nz)]
    barrier = pltpu.get_barrier_semaphore()
    for peer in peers:
        pl.semaphore_signal(barrier, inc=1, device_id=(peer,), device_id_type=MESH)
    pl.semaphore_wait(barrier, len(peers))

    def taps_copy(i, z, dev):
        return remote(taps.at[pl.ds(rows - seg, seg), lanes(z, i)], tb.at[i], tb_s.at[i], tb_r.at[i], dev)

    def hist_copy(i, z, dev):
        return remote(hist.at[pl.ds(0, seg), lanes(z, i)], ha.at[i], ha_s.at[i], ha_r.at[i], dev)

    has_next, has_prev = me < n - 1, me > 0
    for i in range(nz):
        @pl.when(has_next)
        def _(i=i):
            taps_copy(i, (me + 1) // PLANE, me + 1).start()

        @pl.when(has_prev)
        def _(i=i):
            hist_copy(i, (me - 1) // PLANE, me - 1).start()

    def forward(value):
        both = jnp.concatenate(split(value), axis=0)
        spec = jnp.dot(fh[...], both, preferred_element_type=F32) + jnp.dot(
            fl[...], both, preferred_element_type=F32
        )
        return spec[:seg], spec[seg:]

    def keep(ref, i, spec):
        ref[i, :seg], ref[i, seg:] = spec

    def held(ref, i):
        return ref[i, :seg], ref[i, seg:]

    @pl.when(me == 0)
    def _():
        tb[...] = jnp.zeros_like(tb)

    @pl.when(me == n - 1)
    def _():
        ha[...] = jnp.zeros_like(ha)

    for i in range(nz):
        loads[2 * i].wait()
        loads[2 * i + 1].wait()
        hs = [forward(hist_v[i, pl.ds(a * seg, seg)]) for a in range(count)]
        ts = [forward(taps_v[i, pl.ds(a * seg, seg)]) for a in range(count)]
        first, second = local_products(hs, ts)
        keep(sh0, i, hs[0])
        keep(sh1, i, hs[1])
        keep(st1, i, ts[-2])
        keep(q0, i, first)
        keep(q1, i, second)

    contract = (((1,), (1,)), ((), ()))

    def dot_t(a, b):
        return lax.dot_general(a, b, contract, preferred_element_type=F32)

    f, s = fresh[...], self_taps[...]
    both = jnp.concatenate(split(jnp.concatenate([f[:, :seg], f[:, seg:], s[:, :seg], s[:, seg:]], axis=0)), axis=1)
    spec = dot_t(both, fh[...]) + dot_t(both, fl[...])
    pieces = [(spec[k * block : (k + 1) * block, :seg], spec[k * block : (k + 1) * block, seg:]) for k in range(4)]
    a, b = own_products(*pieces)
    high, low_half = split(jnp.concatenate([jnp.concatenate(a, axis=1), jnp.concatenate(b, axis=1)], axis=0))
    res = dot_t(high, gh[...]) + dot_t(low_half, gh[...]) + dot_t(high, gl[...])
    own = jnp.concatenate([res[:block], res[block:]], axis=1)

    def inverse(spec):
        hi, lo = split(jnp.concatenate(spec, axis=0))
        return (
            jnp.dot(gh[...], hi, preferred_element_type=F32)
            + jnp.dot(gh[...], lo, preferred_element_type=F32)
            + jnp.dot(gl[...], hi, preferred_element_type=F32)
        ).T

    def chip_copy(i):
        return remote(parts.at[i, 1 - core], d_recv.at[i], d_s.at[i], d_r.at[i], partner)

    def plane_copy(i, j):
        other, dev = plane_peer(j)
        return remote(p_send.at[i, other], p_recv.at[i, j - 1], p_s.at[i, j - 1], p_r.at[i, j - 1], dev)

    def z_copy(i):
        return remote(z_send.at[i], z_recv.at[i], z_s.at[i], z_r.at[i], (me + (i + 1) * PLANE) % n)

    def step_compute(i):
        @pl.when(has_prev)
        def _():
            taps_copy(i, my_z, me).wait_recv()

        @pl.when(has_next)
        def _():
            hist_copy(i, my_z, me).wait_recv()

        first, second = halo_products(
            held(q0, i), held(q1, i), held(sh0, i), held(sh1, i), held(st1, i), forward(tb[i]), forward(ha[i])
        )
        for half, spec in enumerate((first, second)):
            res = inverse(spec)
            for p in range(chips):
                for c in range(2):
                    at = (p * 2 + c) * block
                    parts[i, c, p, :, pl.ds(half * seg, seg)] = res[at : at + block]
        chip_copy(i).start()

    def step_plane(i):
        chip_copy(i).wait_recv()
        p_send[i] = parts[i, core] + d_recv[i]
        for j in range(1, chips):
            plane_copy(i, j).start()

    def step_z(i):
        for j in range(1, chips):
            plane_copy(i, j).wait_recv()
        total = p_send[i, spot]
        for j in range(1, chips):
            total = total + p_recv[i, j - 1]
        z_send[i] = total
        if i < nz - 1:
            z_copy(i).start()

    for i in range(nz + 2):
        if i < nz:
            step_compute(i)
        if 0 <= i - 1 < nz:
            step_plane(i - 1)
        if 0 <= i - 2 < nz:
            step_z(i - 2)

    total = z_send[nz - 1]
    for i in range(nz - 1):
        z_copy(i).wait_recv()
        total = total + z_recv[i]
    out[...] = gate[...] * (total + own)

    for i in range(nz):
        @pl.when(has_next)
        def _(i=i):
            taps_copy(i, (me + 1) // PLANE, me + 1).wait_send()

        @pl.when(has_prev)
        def _(i=i):
            hist_copy(i, (me - 1) // PLANE, me - 1).wait_send()

        chip_copy(i).wait_send()
        for j in range(1, chips):
            plane_copy(i, j).wait_send()
        if i < nz - 1:
            z_copy(i).wait_send()


def kernel_body(history, taps, self_taps, fresh, gate):
    n = lax.axis_size(AXIS)
    rows, channels = history.shape
    block, new_len = fresh.shape
    seg = new_len // 2
    nz = n // PLANE
    width = channels // nz
    fh, fl = halves(dft_matrix(seg))
    gh, gl = halves(dft_matrix(seg).T / seg)
    fh, fl = np.concatenate([fh, fh], axis=1), np.concatenate([fl, fl], axis=1)
    vmem = pl.BlockSpec(memory_space=pltpu.VMEM)
    hbm = pl.BlockSpec(memory_space=pl.ANY)
    chips = PLANE // 2
    dma = pltpu.SemaphoreType.DMA
    spec = pltpu.VMEM((nz, 2 * seg, width), F32)
    return pl.pallas_call(
        lambda *refs: kernel(n, seg, *refs),
        out_shape=jax.ShapeDtypeStruct(fresh.shape, F32),
        in_specs=[hbm, hbm] + [vmem] * 7,
        out_specs=vmem,
        scratch_shapes=[
            pltpu.VMEM((nz, rows, width), F32),
            pltpu.VMEM((nz, rows, width), F32),
            pltpu.VMEM((nz, seg, width), F32),
            pltpu.VMEM((nz, seg, width), F32),
            spec, spec, spec, spec, spec,
            pltpu.VMEM((nz, 2, chips, block, new_len), F32),
            pltpu.VMEM((nz, chips, block, new_len), F32),
            pltpu.VMEM((nz, chips, block, new_len), F32),
            pltpu.VMEM((nz, chips - 1, block, new_len), F32),
            pltpu.VMEM((nz, block, new_len), F32),
            pltpu.VMEM((nz - 1, block, new_len), F32),
            dma((2, nz)),
            dma((nz,)), dma((nz,)), dma((nz,)), dma((nz,)),
            dma((nz,)), dma((nz,)),
            dma((nz, chips - 1)), dma((nz, chips - 1)),
            dma((nz - 1,)), dma((nz - 1,)),
        ],
        compiler_params=pltpu.CompilerParams(collective_id=0, has_side_effects=True),
        name="hyena",
    )(history, taps, self_taps, fresh, gate, *(jnp.asarray(m) for m in (fh, fl, gh, gl)))


def solution(mesh):
    n = mesh.shape[AXIS]

    def body(history, taps, self_taps, fresh, gate):
        channels = history.shape[1]
        block = fresh.shape[0]
        fits = n % PLANE == 0 and n > PLANE and block % 8 == 0 and (block * PLANE) % 128 == 0
        chosen = kernel_body if fits and channels == block * n else plain_body
        return chosen(history, taps, self_taps, fresh, gate)

    spec = P(AXIS, None)
    return jax.shard_map(body, mesh=mesh, in_specs=(spec,) * 5, out_specs=spec, check_vma=False)
```

```python
import math

import jax
import jax.numpy as jnp
import numpy as np
from jax import lax
from jax.experimental import pallas as pl
from jax.experimental.pallas import tpu as pltpu
from jax.sharding import PartitionSpec as P

AXIS = "seq"
PLANE = 8
MESH = pl.DeviceIdType.MESH
F32 = jnp.float32
BF16 = jnp.bfloat16


def dft_matrix(seg):
    phase = np.outer(4 * np.arange(seg) + 1, np.arange(seg)) % (4 * seg)
    angle = phase * (math.pi / (2 * seg))
    return np.concatenate([np.cos(angle), -np.sin(angle)], axis=0)


def halves(matrix):
    high = np.asarray(matrix, np.float32).astype(BF16)
    low = np.asarray(matrix - high.astype(np.float64), np.float32).astype(BF16)
    return high, low


def split(value):
    high = value.astype(BF16)
    return high, (value - high.astype(F32)).astype(BF16)


def mul_conj(a, b):
    return a[0] * b[0] + a[1] * b[1], a[1] * b[0] - a[0] * b[1]


def mul(a, b):
    return a[0] * b[0] - a[1] * b[1], a[0] * b[1] + a[1] * b[0]


def add(a, b):
    return a[0] + b[0], a[1] + b[1]


def turn(a):
    return -a[1], a[0]


def back(a):
    return a[1], -a[0]


def local_products(hs, ts):
    us = [None] + [add(ts[a], turn(ts[a - 1])) for a in range(1, len(ts))]
    first = mul_conj(hs[0], ts[0])
    for a in range(1, len(hs)):
        first = add(first, mul_conj(hs[a], us[a]))
    second = mul_conj(hs[1], ts[0])
    for a in range(2, len(hs)):
        second = add(second, mul_conj(hs[a], us[a - 1]))
    return first, second


def halo_products(first, second, h0, h1, t_near, t_before, h_after):
    one = mul_conj(h0, t_before)
    two = add(mul_conj(h1, t_before), mul_conj(h_after, t_near))
    return add(first, back(one)), add(add(second, one), back(two))


def own_products(f0, f1, s0, s1):
    first = mul(f0, s0)
    return first, add(turn(first), add(mul(f0, s1), mul(f1, s0)))


def plain_body(history, taps, self_taps, fresh, gate):
    n = lax.axis_size(AXIS)
    seg = fresh.shape[1] // 2
    matrix = jnp.asarray(dft_matrix(seg).astype(np.float32))
    hp = lax.Precision.HIGHEST
    before = lax.ppermute(taps[-seg:], AXIS, [(s, s + 1) for s in range(n - 1)])
    after = lax.ppermute(history[:seg], AXIS, [(s, s - 1) for s in range(1, n)])

    def forward(rows):
        spec = jnp.dot(matrix, rows, precision=hp)
        return spec[:seg], spec[seg:]

    def inverse(spec):
        return jnp.dot(matrix.T / seg, jnp.concatenate(spec, axis=0), precision=hp)

    count = history.shape[0] // seg
    hs = [forward(history[a * seg : (a + 1) * seg]) for a in range(count)]
    ts = [forward(taps[a * seg : (a + 1) * seg]) for a in range(count)]
    first, second = local_products(hs, ts)
    first, second = halo_products(first, second, hs[0], hs[1], ts[-2], forward(before), forward(after))
    part = jnp.concatenate([inverse(first), inverse(second)], axis=0).T
    summed = lax.psum_scatter(part, AXIS, scatter_dimension=0, tiled=True)
    f, s = fresh.T, self_taps.T
    own = own_products(forward(f[:seg]), forward(f[seg:]), forward(s[:seg]), forward(s[seg:]))
    own_part = jnp.concatenate([inverse(own[0]), inverse(own[1])], axis=0).T
    return gate * (summed + own_part)


def kernel(n, seg, hist, taps, self_taps_h, fresh_h, gate_h, fh_h, fl_h, gh_h, gl_h, out,
           self_taps, fresh, gate, fh, fl, gh, gl, hist_v, taps_v, tb, ha, sh0, sh1, st1, q0, q1, parts, d_recv, p_send, p_recv, z_send, z_recv,
           small_sem, load_sem, tb_s, tb_r, ha_s, ha_r, d_s, d_r, p_s, p_r, z_s, z_r):
    me = lax.axis_index(AXIS)
    nz = n // PLANE
    my_z, low = me // PLANE, me % PLANE
    core, spot = me % 2, low // 2
    rows = hist.shape[0]
    count = rows // seg
    width = hist.shape[1] // nz
    block = width // PLANE
    partner = me + 1 - 2 * core
    chips = PLANE // 2

    def lanes(z, i):
        return pl.ds(pl.multiple_of(((z + 1 + i) % nz) * width, width), width)

    def plane_peer(j):
        bit0, bit1 = spot % 2, spot // 2
        other = (bit0 + j % 2) % 2 + 2 * ((bit1 + j // 2) % 2)
        return other, me - low + other * 2 + core

    def remote(src, dst, send, recv, dev):
        return pltpu.make_async_remote_copy(
            src_ref=src, dst_ref=dst, send_sem=send, recv_sem=recv, device_id=(dev,), device_id_type=MESH
        )

    has_next, has_prev = me < n - 1, me > 0
    outer = me + 2 * core - 1
    has_outer = (outer >= 0) & (outer < n)
    peers = [partner]
    peers += [plane_peer(j)[1] for j in range(1, chips)]
    peers += [(me + k * PLANE) % n for k in range(1, nz)]
    barrier = pltpu.get_barrier_semaphore()
    @pl.when(has_outer)
    def _():
        pl.semaphore_signal(barrier, inc=1, device_id=(outer,), device_id_type=MESH)

    for peer in peers:
        pl.semaphore_signal(barrier, inc=1, device_id=(peer,), device_id_type=MESH)

    small = [
        pltpu.make_async_copy(src, dst, small_sem.at[k])
        for k, (src, dst) in enumerate((
            (fh_h, fh), (fl_h, fl), (gh_h, gh), (gl_h, gl), (self_taps_h, self_taps), (fresh_h, fresh), (gate_h, gate),
        ))
    ]
    for copy in small:
        copy.start()
    loads = []
    for i in range(nz):
        for k, (src, dst) in enumerate(((hist, hist_v), (taps, taps_v))):
            copy = pltpu.make_async_copy(src.at[:, lanes(my_z, i)], dst.at[i], load_sem.at[k, i])
            copy.start()
            loads.append(copy)

    pl.semaphore_wait(barrier, len(peers) + jnp.where(has_outer, 1, 0))

    def taps_copy(i, z, dev):
        return remote(taps.at[pl.ds(rows - seg, seg), lanes(z, i)], tb.at[i], tb_s.at[i], tb_r.at[i], dev)

    def hist_copy(i, z, dev):
        return remote(hist.at[pl.ds(0, seg), lanes(z, i)], ha.at[i], ha_s.at[i], ha_r.at[i], dev)

    for i in range(nz):
        @pl.when(has_next)
        def _(i=i):
            taps_copy(i, (me + 1) // PLANE, me + 1).start()

        @pl.when(has_prev)
        def _(i=i):
            hist_copy(i, (me - 1) // PLANE, me - 1).start()

    def forward(value):
        both = jnp.concatenate(split(value), axis=0)
        spec = jnp.dot(fh[...], both, preferred_element_type=F32) + jnp.dot(
            fl[...], both, preferred_element_type=F32
        )
        return spec[:seg], spec[seg:]

    def keep(ref, i, spec):
        ref[i, :seg], ref[i, seg:] = spec

    def held(ref, i):
        return ref[i, :seg], ref[i, seg:]

    @pl.when(me == 0)
    def _():
        tb[...] = jnp.zeros_like(tb)

    @pl.when(me == n - 1)
    def _():
        ha[...] = jnp.zeros_like(ha)

    for copy in small:
        copy.wait()
    for i in range(nz):
        loads[2 * i].wait()
        loads[2 * i + 1].wait()
        hs = [forward(hist_v[i, pl.ds(a * seg, seg)]) for a in range(count)]
        ts = [forward(taps_v[i, pl.ds(a * seg, seg)]) for a in range(count)]
        first, second = local_products(hs, ts)
        keep(sh0, i, hs[0])
        keep(sh1, i, hs[1])
        keep(st1, i, ts[-2])
        keep(q0, i, first)
        keep(q1, i, second)

    contract = (((1,), (1,)), ((), ()))

    def dot_t(a, b):
        return lax.dot_general(a, b, contract, preferred_element_type=F32)

    f, s = fresh[...], self_taps[...]
    both = jnp.concatenate(split(jnp.concatenate([f[:, :seg], f[:, seg:], s[:, :seg], s[:, seg:]], axis=0)), axis=1)
    spec = dot_t(both, fh[...]) + dot_t(both, fl[...])
    pieces = [(spec[k * block : (k + 1) * block, :seg], spec[k * block : (k + 1) * block, seg:]) for k in range(4)]
    a, b = own_products(*pieces)
    high, low_half = split(jnp.concatenate([jnp.concatenate(a, axis=1), jnp.concatenate(b, axis=1)], axis=0))
    res = dot_t(high, gh[...]) + dot_t(low_half, gh[...]) + dot_t(high, gl[...])
    own = jnp.concatenate([res[:block], res[block:]], axis=1)

    def inverse(spec):
        hi, lo = split(jnp.concatenate(spec, axis=0))
        return (
            jnp.dot(gh[...], hi, preferred_element_type=F32)
            + jnp.dot(gh[...], lo, preferred_element_type=F32)
            + jnp.dot(gl[...], hi, preferred_element_type=F32)
        ).T

    def chip_copy(i):
        return remote(parts.at[i, 1 - core], d_recv.at[i], d_s.at[i], d_r.at[i], partner)

    def plane_copy(i, j):
        other, dev = plane_peer(j)
        return remote(p_send.at[i, other], p_recv.at[i, j - 1], p_s.at[i, j - 1], p_r.at[i, j - 1], dev)

    def z_copy(i):
        return remote(z_send.at[i], z_recv.at[i], z_s.at[i], z_r.at[i], (me + (i + 1) * PLANE) % n)

    def step_compute(i):
        @pl.when(has_prev)
        def _():
            taps_copy(i, my_z, me).wait_recv()

        @pl.when(has_next)
        def _():
            hist_copy(i, my_z, me).wait_recv()

        first, second = halo_products(
            held(q0, i), held(q1, i), held(sh0, i), held(sh1, i), held(st1, i), forward(tb[i]), forward(ha[i])
        )
        for half, spec in enumerate((first, second)):
            res = inverse(spec)
            for p in range(chips):
                for c in range(2):
                    at = (p * 2 + c) * block
                    parts[i, c, p, :, pl.ds(half * seg, seg)] = res[at : at + block]
        chip_copy(i).start()

    def step_plane(i):
        chip_copy(i).wait_recv()
        p_send[i] = parts[i, core] + d_recv[i]
        for j in range(1, chips):
            plane_copy(i, j).start()

    def step_z(i):
        for j in range(1, chips):
            plane_copy(i, j).wait_recv()
        total = p_send[i, spot]
        for j in range(1, chips):
            total = total + p_recv[i, j - 1]
        z_send[i] = total
        if i < nz - 1:
            z_copy(i).start()

    for i in range(nz + 2):
        if i < nz:
            step_compute(i)
        if 0 <= i - 1 < nz:
            step_plane(i - 1)
        if 0 <= i - 2 < nz:
            step_z(i - 2)

    total = z_send[nz - 1]
    for i in range(nz - 1):
        z_copy(i).wait_recv()
        total = total + z_recv[i]
    out[...] = gate[...] * (total + own)

    for i in range(nz):
        @pl.when(has_next)
        def _(i=i):
            taps_copy(i, (me + 1) // PLANE, me + 1).wait_send()

        @pl.when(has_prev)
        def _(i=i):
            hist_copy(i, (me - 1) // PLANE, me - 1).wait_send()

        chip_copy(i).wait_send()
        for j in range(1, chips):
            plane_copy(i, j).wait_send()
        if i < nz - 1:
            z_copy(i).wait_send()


def kernel_body(history, taps, self_taps, fresh, gate):
    n = lax.axis_size(AXIS)
    rows, channels = history.shape
    block, new_len = fresh.shape
    seg = new_len // 2
    nz = n // PLANE
    width = channels // nz
    fh, fl = halves(dft_matrix(seg))
    gh, gl = halves(dft_matrix(seg).T / seg)
    fh, fl = np.concatenate([fh, fh], axis=1), np.concatenate([fl, fl], axis=1)
    vmem = pl.BlockSpec(memory_space=pltpu.VMEM)
    hbm = pl.BlockSpec(memory_space=pl.ANY)
    chips = PLANE // 2
    dma = pltpu.SemaphoreType.DMA
    spec = pltpu.VMEM((nz, 2 * seg, width), F32)
    return pl.pallas_call(
        lambda *refs: kernel(n, seg, *refs),
        out_shape=pltpu.VMEM(fresh.shape, F32),
        in_specs=[hbm] * 9,
        out_specs=vmem,
        scratch_shapes=[
            pltpu.VMEM(fresh.shape, F32), pltpu.VMEM(fresh.shape, F32), pltpu.VMEM(fresh.shape, F32),
            pltpu.VMEM(fh.shape, BF16), pltpu.VMEM(fh.shape, BF16), pltpu.VMEM(gh.shape, BF16), pltpu.VMEM(gh.shape, BF16),
            pltpu.VMEM((nz, rows, width), F32),
            pltpu.VMEM((nz, rows, width), F32),
            pltpu.VMEM((nz, seg, width), F32),
            pltpu.VMEM((nz, seg, width), F32),
            spec, spec, spec, spec, spec,
            pltpu.VMEM((nz, 2, chips, block, new_len), F32),
            pltpu.VMEM((nz, chips, block, new_len), F32),
            pltpu.VMEM((nz, chips, block, new_len), F32),
            pltpu.VMEM((nz, chips - 1, block, new_len), F32),
            pltpu.VMEM((nz, block, new_len), F32),
            pltpu.VMEM((nz - 1, block, new_len), F32),
            dma((7,)),
            dma((2, nz)),
            dma((nz,)), dma((nz,)), dma((nz,)), dma((nz,)),
            dma((nz,)), dma((nz,)),
            dma((nz, chips - 1)), dma((nz, chips - 1)),
            dma((nz - 1,)), dma((nz - 1,)),
        ],
        compiler_params=pltpu.CompilerParams(collective_id=0, has_side_effects=True),
        name="hyena",
    )(history, taps, self_taps, fresh, gate, *(jnp.asarray(m) for m in (fh, fl, gh, gl)))


def solution(mesh):
    n = mesh.shape[AXIS]

    def body(history, taps, self_taps, fresh, gate):
        channels = history.shape[1]
        block = fresh.shape[0]
        fits = n % PLANE == 0 and n > PLANE and block % 8 == 0 and (block * PLANE) % 128 == 0
        chosen = kernel_body if fits and channels == block * n else plain_body
        return chosen(history, taps, self_taps, fresh, gate)

    spec = P(AXIS, None)
    return jax.shard_map(body, mesh=mesh, in_specs=(spec,) * 5, out_specs=spec, check_vma=False)
```

```python
import math

import jax
import jax.numpy as jnp
import numpy as np
from jax import lax
from jax.experimental import pallas as pl
from jax.experimental.pallas import tpu as pltpu
from jax.sharding import PartitionSpec as P

AXIS = "seq"
DIRECT = 2
PLANE = 8
MESH = pl.DeviceIdType.MESH
F32 = jnp.float32
BF16 = jnp.bfloat16


def dft_matrix(seg):
    phase = np.outer(4 * np.arange(seg) + 1, np.arange(seg)) % (4 * seg)
    angle = phase * (math.pi / (2 * seg))
    return np.concatenate([np.cos(angle), -np.sin(angle)], axis=0)


def halves(matrix):
    high = np.asarray(matrix, np.float32).astype(BF16)
    low = np.asarray(matrix - high.astype(np.float64), np.float32).astype(BF16)
    return high, low


def split(value):
    high = value.astype(BF16)
    return high, (value - high.astype(F32)).astype(BF16)


def mul_conj(a, b):
    return a[0] * b[0] + a[1] * b[1], a[1] * b[0] - a[0] * b[1]


def mul(a, b):
    return a[0] * b[0] - a[1] * b[1], a[0] * b[1] + a[1] * b[0]


def add(a, b):
    return a[0] + b[0], a[1] + b[1]


def turn(a):
    return -a[1], a[0]


def back(a):
    return a[1], -a[0]


def local_products(hs, ts):
    us = [None] + [add(ts[a], turn(ts[a - 1])) for a in range(1, len(ts))]
    first = mul_conj(hs[0], ts[0])
    for a in range(1, len(hs)):
        first = add(first, mul_conj(hs[a], us[a]))
    second = mul_conj(hs[1], ts[0])
    for a in range(2, len(hs)):
        second = add(second, mul_conj(hs[a], us[a - 1]))
    return first, second


def halo_products(first, second, h0, h1, t_near, t_before, h_after):
    one = mul_conj(h0, t_before)
    two = add(mul_conj(h1, t_before), mul_conj(h_after, t_near))
    return add(first, back(one)), add(add(second, one), back(two))


def own_products(f0, f1, s0, s1):
    first = mul(f0, s0)
    return first, add(turn(first), add(mul(f0, s1), mul(f1, s0)))


def plain_body(history, taps, self_taps, fresh, gate):
    n = lax.axis_size(AXIS)
    seg = fresh.shape[1] // 2
    matrix = jnp.asarray(dft_matrix(seg).astype(np.float32))
    hp = lax.Precision.HIGHEST
    before = lax.ppermute(taps[-seg:], AXIS, [(s, s + 1) for s in range(n - 1)])
    after = lax.ppermute(history[:seg], AXIS, [(s, s - 1) for s in range(1, n)])

    def forward(rows):
        spec = jnp.dot(matrix, rows, precision=hp)
        return spec[:seg], spec[seg:]

    def inverse(spec):
        return jnp.dot(matrix.T / seg, jnp.concatenate(spec, axis=0), precision=hp)

    count = history.shape[0] // seg
    hs = [forward(history[a * seg : (a + 1) * seg]) for a in range(count)]
    ts = [forward(taps[a * seg : (a + 1) * seg]) for a in range(count)]
    first, second = local_products(hs, ts)
    first, second = halo_products(first, second, hs[0], hs[1], ts[-2], forward(before), forward(after))
    part = jnp.concatenate([inverse(first), inverse(second)], axis=0).T
    summed = lax.psum_scatter(part, AXIS, scatter_dimension=0, tiled=True)
    f, s = fresh.T, self_taps.T
    own = own_products(forward(f[:seg]), forward(f[seg:]), forward(s[:seg]), forward(s[seg:]))
    own_part = jnp.concatenate([inverse(own[0]), inverse(own[1])], axis=0).T
    return gate * (summed + own_part)


def kernel(n, seg, hist, taps, self_taps_h, fresh_h, gate_h, fh_h, fl_h, gh_h, gl_h, out,
           self_taps, fresh, gate, fh, fl, gh, gl, hist_v, taps_v, tb, ha, sh0, sh1, st1, q0, q1, parts, d_recv, sums, y_send, y_recv, w_send, w_recv,
           p_recv, z_send, z_recv, x_send, x_recv,
           small_sem, load_sem, tb_s, tb_r, ha_s, ha_r, d_s, d_r, y_s, y_r, w_s, w_r,
           p_s, p_r, z_s, z_r, x_s, x_r):
    me = lax.axis_index(AXIS)
    nz = n // PLANE
    my_z, low = me // PLANE, me % PLANE
    core, x, y = me % 2, low // 2 % 2, low // 4
    rows = hist.shape[0]
    count = rows // seg
    width = hist.shape[1] // nz
    block = width // PLANE
    partner = me + 1 - 2 * core
    routed = nz - DIRECT
    last = nz - 1
    half = width // 2
    x_peer, y_peer = me + 2 - 4 * x, me + 4 - 8 * y
    diagonal = me + 2 - 4 * x + 4 - 8 * y
    near = (y_peer, diagonal, x_peer)

    def pieces(i, dev):
        base = ((dev // PLANE + 1 + i) % nz) * width
        if i < last:
            return [(pl.ds(pl.multiple_of(base, width), width), pl.ds(0, width))]
        row = dev % PLANE // 4
        return [
            (pl.ds(pl.multiple_of(base + ((row + 1 + h) % 2) * half, half), half), pl.ds(h * half, half))
            for h in range(2)
        ]

    def remote(src, dst, send, recv, dev):
        return pltpu.make_async_remote_copy(
            src_ref=src, dst_ref=dst, send_sem=send, recv_sem=recv, device_id=(dev,), device_id_type=MESH
        )

    has_next, has_prev = me < n - 1, me > 0
    outer = me + 2 * core - 1
    has_outer = (outer >= 0) & (outer < n)
    peers = [partner]
    peers += near
    peers += [(me + k * PLANE) % n for k in range(1, nz)]
    barrier = pltpu.get_barrier_semaphore()
    @pl.when(has_outer)
    def _():
        pl.semaphore_signal(barrier, inc=1, device_id=(outer,), device_id_type=MESH)

    for peer in peers:
        pl.semaphore_signal(barrier, inc=1, device_id=(peer,), device_id_type=MESH)

    small = [
        pltpu.make_async_copy(src, dst, small_sem.at[k])
        for k, (src, dst) in enumerate((
            (fh_h, fh), (fl_h, fl), (gh_h, gh), (gl_h, gl), (self_taps_h, self_taps), (fresh_h, fresh), (gate_h, gate),
        ))
    ]
    for copy in small:
        copy.start()
    loads = [[] for _ in range(nz)]
    for i in range(nz):
        for k, (src, dst) in enumerate(((hist, hist_v), (taps, taps_v))):
            for h, (here, there) in enumerate(pieces(i, me)):
                copy = pltpu.make_async_copy(src.at[:, here], dst.at[i, :, there], load_sem.at[k, i + h])
                copy.start()
                loads[i].append(copy)

    pl.semaphore_wait(barrier, len(peers) + jnp.where(has_outer, 1, 0))

    def taps_copies(i, dev):
        return [
            remote(taps.at[pl.ds(rows - seg, seg), here], tb.at[i, :, there], tb_s.at[i + h], tb_r.at[i + h], dev)
            for h, (here, there) in enumerate(pieces(i, dev))
        ]

    def hist_copies(i, dev):
        return [
            remote(hist.at[pl.ds(0, seg), here], ha.at[i, :, there], ha_s.at[i + h], ha_r.at[i + h], dev)
            for h, (here, there) in enumerate(pieces(i, dev))
        ]

    for i in range(nz):
        @pl.when(has_next)
        def _(i=i):
            for copy in taps_copies(i, me + 1):
                copy.start()

        @pl.when(has_prev)
        def _(i=i):
            for copy in hist_copies(i, me - 1):
                copy.start()

    def forward(value):
        both = jnp.concatenate(split(value), axis=0)
        spec = jnp.dot(fh[...], both, preferred_element_type=F32) + jnp.dot(
            fl[...], both, preferred_element_type=F32
        )
        return spec[:seg], spec[seg:]

    def keep(ref, i, spec):
        ref[i, :seg], ref[i, seg:] = spec

    def held(ref, i, at):
        return ref[i, :seg, at], ref[i, seg:, at]

    @pl.when(me == 0)
    def _():
        tb[...] = jnp.zeros_like(tb)

    @pl.when(me == n - 1)
    def _():
        ha[...] = jnp.zeros_like(ha)

    for copy in small:
        copy.wait()
    for i in range(nz):
        for copy in loads[i]:
            copy.wait()
        hs = [forward(hist_v[i, pl.ds(a * seg, seg)]) for a in range(count)]
        ts = [forward(taps_v[i, pl.ds(a * seg, seg)]) for a in range(count)]
        first, second = local_products(hs, ts)
        keep(sh0, i, hs[0])
        keep(sh1, i, hs[1])
        keep(st1, i, ts[-2])
        keep(q0, i, first)
        keep(q1, i, second)

    contract = (((1,), (1,)), ((), ()))

    def dot_t(a, b):
        return lax.dot_general(a, b, contract, preferred_element_type=F32)

    f, s = fresh[...], self_taps[...]
    both = jnp.concatenate(split(jnp.concatenate([f[:, :seg], f[:, seg:], s[:, :seg], s[:, seg:]], axis=0)), axis=1)
    spec = dot_t(both, fh[...]) + dot_t(both, fl[...])
    quads = [(spec[k * block : (k + 1) * block, :seg], spec[k * block : (k + 1) * block, seg:]) for k in range(4)]
    a, b = own_products(*quads)
    high, low_half = split(jnp.concatenate([jnp.concatenate(a, axis=1), jnp.concatenate(b, axis=1)], axis=0))
    res = dot_t(high, gh[...]) + dot_t(low_half, gh[...]) + dot_t(high, gl[...])
    own = jnp.concatenate([res[:block], res[block:]], axis=1)

    def inverse(spec):
        hi, lo = split(jnp.concatenate(spec, axis=0))
        return (
            jnp.dot(gh[...], hi, preferred_element_type=F32)
            + jnp.dot(gh[...], lo, preferred_element_type=F32)
            + jnp.dot(gl[...], hi, preferred_element_type=F32)
        ).T

    def chip_copy(i, h=None):
        span, k = (pl.ds(0, 4), i) if h is None else (pl.ds(2 * h, 2), i + h)
        return remote(parts.at[i, 1 - core, span], d_recv.at[i, span], d_s.at[k], d_r.at[k], partner)

    def y_copy(i):
        return remote(y_send.at[i], y_recv.at[i], y_s.at[i], y_r.at[i], y_peer)

    def w_copy(i):
        return remote(w_send.at[i], w_recv.at[i], w_s.at[i], w_r.at[i], (me + (i + 1) * PLANE) % n)

    def near_copy(i, j):
        k = i - routed
        return remote(sums.at[k, (0, 1, 3)[j]], p_recv.at[k, j], p_s.at[k, j], p_r.at[k, j], near[j])

    def z_copy(i):
        k = i - routed
        return remote(z_send.at[k], z_recv.at[k], z_s.at[k], z_r.at[k], (me + (i + 1) * PLANE) % n)

    def x_copy():
        return remote(x_send, x_recv, x_s, x_r, x_peer)

    def compute(i, h=None):
        which = slice(None) if h is None else slice(h, h + 1)

        @pl.when(has_prev)
        def _():
            for copy in taps_copies(i, me)[which]:
                copy.wait_recv()

        @pl.when(has_next)
        def _():
            for copy in hist_copies(i, me)[which]:
                copy.wait_recv()

        at = pl.ds(0, width) if h is None else pl.ds(h * half, half)
        both = halo_products(
            held(q0, i, at), held(q1, i, at), held(sh0, i, at), held(sh1, i, at), held(st1, i, at),
            forward(tb[i, :, at]), forward(ha[i, :, at]),
        )
        for side, spec in enumerate(both):
            res = inverse(spec)
            for k in range(res.shape[0] // block):
                col = k // 2 % 2
                row = (k // 4 + y + 1) % 2 if h is None else h
                place = 2 * row + (col + x) % 2
                parts[i, k % 2, place, :, pl.ds(side * seg, seg)] = res[k * block : (k + 1) * block]
        chip_copy(i, h).start()

    def route_y(i):
        chip_copy(i).wait_recv()
        y_send[i] = parts[i, core, :2] + d_recv[i, :2]
        y_copy(i).start()

    def route_z(i):
        y_copy(i).wait_recv()
        w_send[i] = parts[i, core, 2:] + d_recv[i, 2:] + y_recv[i]
        w_copy(i).start()

    def spread(i, h=None):
        chip_copy(i, h).wait_recv()
        lo, hi = (0, 4) if h is None else (2 * h, 2 * h + 2)
        sums[i - routed, lo:hi] = parts[i, core, lo:hi] + d_recv[i, lo:hi]
        for j, place in enumerate((0, 1, 3)):
            if lo <= place < hi:
                near_copy(i, j).start()

    def gathered(i):
        for j in range(3):
            near_copy(i, j).wait_recv()
        k = i - routed
        return sums[k, 2] + p_recv[k, 0] + p_recv[k, 1] + p_recv[k, 2]

    for i in range(last):
        compute(i)
        if i < routed:
            route_y(i)
        else:
            spread(i)
        if 0 <= i - 1 < routed:
            route_z(i - 1)
    compute(last, 0)
    if routed == last:
        route_z(last - 1)
    spread(last, 0)
    compute(last, 1)
    spread(last, 1)
    for i in range(routed, last):
        z_send[i - routed] = gathered(i)
        z_copy(i).start()
    for i in range(routed):
        w_copy(i).wait_recv()
    merged = w_recv[0]
    for i in range(1, routed):
        merged = merged + w_recv[i]
    x_send[...] = merged[1]
    x_copy().start()
    total = gathered(last) + merged[0]
    for i in range(routed, last):
        z_copy(i).wait_recv()
        total = total + z_recv[i - routed]
    x_copy().wait_recv()
    out[...] = gate[...] * (total + x_recv[...] + own)

    x_copy().wait_send()
    for i in range(nz):
        @pl.when(has_next)
        def _(i=i):
            for copy in taps_copies(i, me + 1):
                copy.wait_send()

        @pl.when(has_prev)
        def _(i=i):
            for copy in hist_copies(i, me - 1):
                copy.wait_send()

        for h in (None,) if i < last else (0, 1):
            chip_copy(i, h).wait_send()
        if i < routed:
            y_copy(i).wait_send()
            w_copy(i).wait_send()
        else:
            for j in range(3):
                near_copy(i, j).wait_send()
            if i < last:
                z_copy(i).wait_send()


def kernel_body(history, taps, self_taps, fresh, gate):
    n = lax.axis_size(AXIS)
    rows, channels = history.shape
    block, new_len = fresh.shape
    seg = new_len // 2
    nz = n // PLANE
    width = channels // nz
    fh, fl = halves(dft_matrix(seg))
    gh, gl = halves(dft_matrix(seg).T / seg)
    fh, fl = np.concatenate([fh, fh], axis=1), np.concatenate([fl, fl], axis=1)
    vmem = pl.BlockSpec(memory_space=pltpu.VMEM)
    hbm = pl.BlockSpec(memory_space=pl.ANY)
    chips = PLANE // 2
    dma = pltpu.SemaphoreType.DMA
    spec = pltpu.VMEM((nz, 2 * seg, width), F32)
    pair = pltpu.VMEM((nz - DIRECT, 2, block, new_len), F32)
    return pl.pallas_call(
        lambda *refs: kernel(n, seg, *refs),
        out_shape=pltpu.VMEM(fresh.shape, F32),
        in_specs=[hbm] * 9,
        out_specs=vmem,
        scratch_shapes=[
            pltpu.VMEM(fresh.shape, F32), pltpu.VMEM(fresh.shape, F32), pltpu.VMEM(fresh.shape, F32),
            pltpu.VMEM(fh.shape, BF16), pltpu.VMEM(fh.shape, BF16), pltpu.VMEM(gh.shape, BF16), pltpu.VMEM(gh.shape, BF16),
            pltpu.VMEM((nz, rows, width), F32),
            pltpu.VMEM((nz, rows, width), F32),
            pltpu.VMEM((nz, seg, width), F32),
            pltpu.VMEM((nz, seg, width), F32),
            spec, spec, spec, spec, spec,
            pltpu.VMEM((nz, 2, chips, block, new_len), F32),
            pltpu.VMEM((nz, chips, block, new_len), F32),
            pltpu.VMEM((DIRECT, chips, block, new_len), F32),
            pair, pair, pair, pair,
            pltpu.VMEM((DIRECT, 3, block, new_len), F32),
            pltpu.VMEM((DIRECT, block, new_len), F32),
            pltpu.VMEM((DIRECT, block, new_len), F32),
            pltpu.VMEM((block, new_len), F32),
            pltpu.VMEM((block, new_len), F32),
            dma((7,)),
            dma((2, nz + 1)),
            dma((nz + 1,)), dma((nz + 1,)), dma((nz + 1,)), dma((nz + 1,)),
            dma((nz + 1,)), dma((nz + 1,)),
            dma((nz,)), dma((nz,)), dma((nz,)), dma((nz,)),
            dma((DIRECT, 3)), dma((DIRECT, 3)),
            dma((DIRECT,)), dma((DIRECT,)),
            dma, dma,
        ],
        compiler_params=pltpu.CompilerParams(collective_id=0, has_side_effects=True),
        name="hyena",
    )(history, taps, self_taps, fresh, gate, *(jnp.asarray(m) for m in (fh, fl, gh, gl)))


def solution(mesh):
    n = mesh.shape[AXIS]

    def body(history, taps, self_taps, fresh, gate):
        channels = history.shape[1]
        block = fresh.shape[0]
        fits = n % PLANE == 0 and n > DIRECT * PLANE and block % 8 == 0 and (block * PLANE) % 256 == 0
        chosen = kernel_body if fits and channels == block * n else plain_body
        return chosen(history, taps, self_taps, fresh, gate)

    spec = P(AXIS, None)
    return jax.shard_map(body, mesh=mesh, in_specs=(spec,) * 5, out_specs=spec, check_vma=False)
```

```python
import math

import jax
import jax.numpy as jnp
import numpy as np
from jax import lax
from jax.experimental import pallas as pl
from jax.experimental.pallas import tpu as pltpu
from jax.sharding import PartitionSpec as P

AXIS = "seq"
AHEAD = 3
DIRECT = 3
PLANE = 8
MESH = pl.DeviceIdType.MESH
F32 = jnp.float32
BF16 = jnp.bfloat16


def dft_matrix(seg):
    phase = np.outer(4 * np.arange(seg) + 1, np.arange(seg)) % (4 * seg)
    angle = phase * (math.pi / (2 * seg))
    return np.concatenate([np.cos(angle), -np.sin(angle)], axis=0)


def halves(matrix):
    high = np.asarray(matrix, np.float32).astype(BF16)
    low = np.asarray(matrix - high.astype(np.float64), np.float32).astype(BF16)
    return high, low


def split(value):
    high = value.astype(BF16)
    return high, (value - high.astype(F32)).astype(BF16)


def mul_conj(a, b):
    return a[0] * b[0] + a[1] * b[1], a[1] * b[0] - a[0] * b[1]


def mul(a, b):
    return a[0] * b[0] - a[1] * b[1], a[0] * b[1] + a[1] * b[0]


def add(a, b):
    return a[0] + b[0], a[1] + b[1]


def turn(a):
    return -a[1], a[0]


def back(a):
    return a[1], -a[0]


def local_products(hs, ts):
    us = [None] + [add(ts[a], turn(ts[a - 1])) for a in range(1, len(ts))]
    first = mul_conj(hs[0], ts[0])
    for a in range(1, len(hs)):
        first = add(first, mul_conj(hs[a], us[a]))
    second = mul_conj(hs[1], ts[0])
    for a in range(2, len(hs)):
        second = add(second, mul_conj(hs[a], us[a - 1]))
    return first, second


def halo_products(first, second, h0, h1, t_near, t_before, h_after):
    one = mul_conj(h0, t_before)
    two = add(mul_conj(h1, t_before), mul_conj(h_after, t_near))
    return add(first, back(one)), add(add(second, one), back(two))


def own_products(f0, f1, s0, s1):
    first = mul(f0, s0)
    return first, add(turn(first), add(mul(f0, s1), mul(f1, s0)))


def plain_body(history, taps, self_taps, fresh, gate):
    n = lax.axis_size(AXIS)
    seg = fresh.shape[1] // 2
    matrix = jnp.asarray(dft_matrix(seg).astype(np.float32))
    hp = lax.Precision.HIGHEST
    before = lax.ppermute(taps[-seg:], AXIS, [(s, s + 1) for s in range(n - 1)])
    after = lax.ppermute(history[:seg], AXIS, [(s, s - 1) for s in range(1, n)])

    def forward(rows):
        spec = jnp.dot(matrix, rows, precision=hp)
        return spec[:seg], spec[seg:]

    def inverse(spec):
        return jnp.dot(matrix.T / seg, jnp.concatenate(spec, axis=0), precision=hp)

    count = history.shape[0] // seg
    hs = [forward(history[a * seg : (a + 1) * seg]) for a in range(count)]
    ts = [forward(taps[a * seg : (a + 1) * seg]) for a in range(count)]
    first, second = local_products(hs, ts)
    first, second = halo_products(first, second, hs[0], hs[1], ts[-2], forward(before), forward(after))
    part = jnp.concatenate([inverse(first), inverse(second)], axis=0).T
    summed = lax.psum_scatter(part, AXIS, scatter_dimension=0, tiled=True)
    f, s = fresh.T, self_taps.T
    own = own_products(forward(f[:seg]), forward(f[seg:]), forward(s[:seg]), forward(s[seg:]))
    own_part = jnp.concatenate([inverse(own[0]), inverse(own[1])], axis=0).T
    return gate * (summed + own_part)


def kernel(n, seg, hist, taps, self_taps_h, fresh_h, gate_h, fh_h, fl_h, gh_h, gl_h, out,
           self_taps, fresh, gate, fh, fl, gh, gl, hist_v, taps_v, tb, ha, sh0, sh1, st1, q0, q1, parts, d_recv, sums, y_send, y_recv, w_send, w_recv,
           p_recv, z_send, z_recv, x_send, x_recv,
           small_sem, load_sem, tb_s, tb_r, ha_s, ha_r, d_s, d_r, y_s, y_r, w_s, w_r,
           p_s, p_r, z_s, z_r, x_s, x_r):
    me = lax.axis_index(AXIS)
    nz = n // PLANE
    my_z, low = me // PLANE, me % PLANE
    core, x, y = me % 2, low // 2 % 2, low // 4
    rows = hist.shape[0]
    count = rows // seg
    width = hist.shape[1] // nz
    block = width // PLANE
    partner = me + 1 - 2 * core
    routed = nz - DIRECT
    last = nz - 1
    half = width // 2
    x_peer, y_peer = me + 2 - 4 * x, me + 4 - 8 * y
    diagonal = me + 2 - 4 * x + 4 - 8 * y
    near = (y_peer, diagonal, x_peer)

    def pieces(i, dev):
        base = ((dev // PLANE + 1 + i) % nz) * width
        if i < last:
            return [(pl.ds(pl.multiple_of(base, width), width), pl.ds(0, width))]
        row = dev % PLANE // 4
        return [
            (pl.ds(pl.multiple_of(base + ((row + 1 + h) % 2) * half, half), half), pl.ds(h * half, half))
            for h in range(2)
        ]

    def remote(src, dst, send, recv, dev):
        return pltpu.make_async_remote_copy(
            src_ref=src, dst_ref=dst, send_sem=send, recv_sem=recv, device_id=(dev,), device_id_type=MESH
        )

    has_next, has_prev = me < n - 1, me > 0
    outer = me + 2 * core - 1
    has_outer = (outer >= 0) & (outer < n)
    peers = [partner]
    peers += near
    peers += [(me + k * PLANE) % n for k in range(1, nz)]
    barrier = pltpu.get_barrier_semaphore()
    @pl.when(has_outer)
    def _():
        pl.semaphore_signal(barrier, inc=1, device_id=(outer,), device_id_type=MESH)

    for peer in peers:
        pl.semaphore_signal(barrier, inc=1, device_id=(peer,), device_id_type=MESH)

    small = [
        pltpu.make_async_copy(src, dst, small_sem.at[k])
        for k, (src, dst) in enumerate((
            (fh_h, fh), (fl_h, fl), (gh_h, gh), (gl_h, gl), (self_taps_h, self_taps), (fresh_h, fresh), (gate_h, gate),
        ))
    ]
    for copy in small:
        copy.start()
    loads = [[] for _ in range(nz)]
    for i in range(nz):
        for k, (src, dst) in enumerate(((hist, hist_v), (taps, taps_v))):
            for h, (here, there) in enumerate(pieces(i, me)):
                copy = pltpu.make_async_copy(src.at[:, here], dst.at[i, :, there], load_sem.at[k, i + h])
                copy.start()
                loads[i].append(copy)

    pl.semaphore_wait(barrier, len(peers) + jnp.where(has_outer, 1, 0))

    def taps_copies(i, dev):
        return [
            remote(taps.at[pl.ds(rows - seg, seg), here], tb.at[i, :, there], tb_s.at[i + h], tb_r.at[i + h], dev)
            for h, (here, there) in enumerate(pieces(i, dev))
        ]

    def hist_copies(i, dev):
        return [
            remote(hist.at[pl.ds(0, seg), here], ha.at[i, :, there], ha_s.at[i + h], ha_r.at[i + h], dev)
            for h, (here, there) in enumerate(pieces(i, dev))
        ]

    def send_halo(i):
        @pl.when(has_next)
        def _():
            for copy in taps_copies(i, me + 1):
                copy.start()

        @pl.when(has_prev)
        def _():
            for copy in hist_copies(i, me - 1):
                copy.start()

    for i in range(min(AHEAD, nz)):
        send_halo(i)

    def forward(value):
        both = jnp.concatenate(split(value), axis=0)
        spec = jnp.dot(fh[...], both, preferred_element_type=F32) + jnp.dot(
            fl[...], both, preferred_element_type=F32
        )
        return spec[:seg], spec[seg:]

    def keep(ref, i, spec):
        ref[i, :seg], ref[i, seg:] = spec

    def held(ref, i, at):
        return ref[i, :seg, at], ref[i, seg:, at]

    @pl.when(me == 0)
    def _():
        tb[...] = jnp.zeros_like(tb)

    @pl.when(me == n - 1)
    def _():
        ha[...] = jnp.zeros_like(ha)

    for copy in small:
        copy.wait()
    for i in range(nz):
        for copy in loads[i]:
            copy.wait()
        hs = [forward(hist_v[i, pl.ds(a * seg, seg)]) for a in range(count)]
        ts = [forward(taps_v[i, pl.ds(a * seg, seg)]) for a in range(count)]
        first, second = local_products(hs, ts)
        keep(sh0, i, hs[0])
        keep(sh1, i, hs[1])
        keep(st1, i, ts[-2])
        keep(q0, i, first)
        keep(q1, i, second)

    contract = (((1,), (1,)), ((), ()))

    def dot_t(a, b):
        return lax.dot_general(a, b, contract, preferred_element_type=F32)

    f, s = fresh[...], self_taps[...]
    both = jnp.concatenate(split(jnp.concatenate([f[:, :seg], f[:, seg:], s[:, :seg], s[:, seg:]], axis=0)), axis=1)
    spec = dot_t(both, fh[...]) + dot_t(both, fl[...])
    quads = [(spec[k * block : (k + 1) * block, :seg], spec[k * block : (k + 1) * block, seg:]) for k in range(4)]
    a, b = own_products(*quads)
    high, low_half = split(jnp.concatenate([jnp.concatenate(a, axis=1), jnp.concatenate(b, axis=1)], axis=0))
    res = dot_t(high, gh[...]) + dot_t(low_half, gh[...]) + dot_t(high, gl[...])
    own = jnp.concatenate([res[:block], res[block:]], axis=1)

    def inverse(spec):
        hi, lo = split(jnp.concatenate(spec, axis=0))
        return (
            jnp.dot(gh[...], hi, preferred_element_type=F32)
            + jnp.dot(gh[...], lo, preferred_element_type=F32)
            + jnp.dot(gl[...], hi, preferred_element_type=F32)
        ).T

    def chip_copy(i, h=None):
        span, k = (pl.ds(0, 4), i) if h is None else (pl.ds(2 * h, 2), i + h)
        return remote(parts.at[i, 1 - core, span], d_recv.at[i, span], d_s.at[k], d_r.at[k], partner)

    def y_copy(i):
        return remote(y_send.at[i], y_recv.at[i], y_s.at[i], y_r.at[i], y_peer)

    def w_copy(i):
        return remote(w_send.at[i], w_recv.at[i], w_s.at[i], w_r.at[i], (me + (i + 1) * PLANE) % n)

    def near_copy(i, j):
        k = i - routed
        return remote(sums.at[k, (0, 1, 3)[j]], p_recv.at[k, j], p_s.at[k, j], p_r.at[k, j], near[j])

    def z_copy(i):
        k = i - routed
        return remote(z_send.at[k], z_recv.at[k], z_s.at[k], z_r.at[k], (me + (i + 1) * PLANE) % n)

    def x_copy():
        return remote(x_send, x_recv, x_s, x_r, x_peer)

    def compute(i, h=None):
        which = slice(None) if h is None else slice(h, h + 1)

        @pl.when(has_prev)
        def _():
            for copy in taps_copies(i, me)[which]:
                copy.wait_recv()

        @pl.when(has_next)
        def _():
            for copy in hist_copies(i, me)[which]:
                copy.wait_recv()

        at = pl.ds(0, width) if h is None else pl.ds(h * half, half)
        both = halo_products(
            held(q0, i, at), held(q1, i, at), held(sh0, i, at), held(sh1, i, at), held(st1, i, at),
            forward(tb[i, :, at]), forward(ha[i, :, at]),
        )
        for side, spec in enumerate(both):
            res = inverse(spec)
            for k in range(res.shape[0] // block):
                col = k // 2 % 2
                row = (k // 4 + y + 1) % 2 if h is None else h
                place = 2 * row + (col + x) % 2
                parts[i, k % 2, place, :, pl.ds(side * seg, seg)] = res[k * block : (k + 1) * block]
        chip_copy(i, h).start()

    def route_y(i):
        chip_copy(i).wait_recv()
        y_send[i] = parts[i, core, :2] + d_recv[i, :2]
        y_copy(i).start()

    def route_z(i):
        y_copy(i).wait_recv()
        w_send[i] = parts[i, core, 2:] + d_recv[i, 2:] + y_recv[i]
        w_copy(i).start()

    def spread(i, h=None):
        chip_copy(i, h).wait_recv()
        lo, hi = (0, 4) if h is None else (2 * h, 2 * h + 2)
        sums[i - routed, lo:hi] = parts[i, core, lo:hi] + d_recv[i, lo:hi]
        for j, place in enumerate((0, 1, 3)):
            if lo <= place < hi:
                near_copy(i, j).start()

    def gathered(i):
        for j in range(3):
            near_copy(i, j).wait_recv()
        k = i - routed
        return sums[k, 2] + p_recv[k, 0] + p_recv[k, 1] + p_recv[k, 2]

    for i in range(last):
        compute(i)
        if i < routed:
            route_y(i)
        else:
            spread(i)
        if i + AHEAD < nz:
            send_halo(i + AHEAD)
        if 0 <= i - 1 < routed:
            route_z(i - 1)
    compute(last, 0)
    if routed == last:
        route_z(last - 1)
    spread(last, 0)
    compute(last, 1)
    spread(last, 1)
    for i in range(routed, last):
        z_send[i - routed] = gathered(i)
        z_copy(i).start()
    for i in range(routed):
        w_copy(i).wait_recv()
    total = gathered(last)
    if routed:
        merged = w_recv[0]
        for i in range(1, routed):
            merged = merged + w_recv[i]
        x_send[...] = merged[1]
        x_copy().start()
        total = total + merged[0]
    for i in range(routed, last):
        z_copy(i).wait_recv()
        total = total + z_recv[i - routed]
    if routed:
        x_copy().wait_recv()
        total = total + x_recv[...]
        x_copy().wait_send()
    out[...] = gate[...] * (total + own)

    for i in range(nz):
        @pl.when(has_next)
        def _(i=i):
            for copy in taps_copies(i, me + 1):
                copy.wait_send()

        @pl.when(has_prev)
        def _(i=i):
            for copy in hist_copies(i, me - 1):
                copy.wait_send()

        for h in (None,) if i < last else (0, 1):
            chip_copy(i, h).wait_send()
        if i < routed:
            y_copy(i).wait_send()
            w_copy(i).wait_send()
        else:
            for j in range(3):
                near_copy(i, j).wait_send()
            if i < last:
                z_copy(i).wait_send()


def kernel_body(history, taps, self_taps, fresh, gate):
    n = lax.axis_size(AXIS)
    rows, channels = history.shape
    block, new_len = fresh.shape
    seg = new_len // 2
    nz = n // PLANE
    width = channels // nz
    fh, fl = halves(dft_matrix(seg))
    gh, gl = halves(dft_matrix(seg).T / seg)
    fh, fl = np.concatenate([fh, fh], axis=1), np.concatenate([fl, fl], axis=1)
    vmem = pl.BlockSpec(memory_space=pltpu.VMEM)
    hbm = pl.BlockSpec(memory_space=pl.ANY)
    chips = PLANE // 2
    dma = pltpu.SemaphoreType.DMA
    spec = pltpu.VMEM((nz, 2 * seg, width), F32)
    pair = pltpu.VMEM((max(nz - DIRECT, 1), 2, block, new_len), F32)
    return pl.pallas_call(
        lambda *refs: kernel(n, seg, *refs),
        out_shape=pltpu.VMEM(fresh.shape, F32),
        in_specs=[hbm] * 9,
        out_specs=vmem,
        scratch_shapes=[
            pltpu.VMEM(fresh.shape, F32), pltpu.VMEM(fresh.shape, F32), pltpu.VMEM(fresh.shape, F32),
            pltpu.VMEM(fh.shape, BF16), pltpu.VMEM(fh.shape, BF16), pltpu.VMEM(gh.shape, BF16), pltpu.VMEM(gh.shape, BF16),
            pltpu.VMEM((nz, rows, width), F32),
            pltpu.VMEM((nz, rows, width), F32),
            pltpu.VMEM((nz, seg, width), F32),
            pltpu.VMEM((nz, seg, width), F32),
            spec, spec, spec, spec, spec,
            pltpu.VMEM((nz, 2, chips, block, new_len), F32),
            pltpu.VMEM((nz, chips, block, new_len), F32),
            pltpu.VMEM((DIRECT, chips, block, new_len), F32),
            pair, pair, pair, pair,
            pltpu.VMEM((DIRECT, 3, block, new_len), F32),
            pltpu.VMEM((DIRECT, block, new_len), F32),
            pltpu.VMEM((DIRECT, block, new_len), F32),
            pltpu.VMEM((block, new_len), F32),
            pltpu.VMEM((block, new_len), F32),
            dma((7,)),
            dma((2, nz + 1)),
            dma((nz + 1,)), dma((nz + 1,)), dma((nz + 1,)), dma((nz + 1,)),
            dma((nz + 1,)), dma((nz + 1,)),
            dma((nz,)), dma((nz,)), dma((nz,)), dma((nz,)),
            dma((DIRECT, 3)), dma((DIRECT, 3)),
            dma((DIRECT,)), dma((DIRECT,)),
            dma, dma,
        ],
        compiler_params=pltpu.CompilerParams(collective_id=0, has_side_effects=True),
        name="hyena",
    )(history, taps, self_taps, fresh, gate, *(jnp.asarray(m) for m in (fh, fl, gh, gl)))


def solution(mesh):
    n = mesh.shape[AXIS]

    def body(history, taps, self_taps, fresh, gate):
        channels = history.shape[1]
        block = fresh.shape[0]
        fits = n % PLANE == 0 and n >= DIRECT * PLANE and block % 8 == 0 and (block * PLANE) % 256 == 0
        chosen = kernel_body if fits and channels == block * n else plain_body
        return chosen(history, taps, self_taps, fresh, gate)

    spec = P(AXIS, None)
    return jax.shard_map(body, mesh=mesh, in_specs=(spec,) * 5, out_specs=spec, check_vma=False)
```

```python
import math

import jax
import jax.numpy as jnp
import numpy as np
from jax import lax
from jax.experimental import pallas as pl
from jax.experimental.pallas import tpu as pltpu
from jax.sharding import PartitionSpec as P

AXIS = "seq"
AHEAD = 3
DIRECT = 3
PLANE = 8
MESH = pl.DeviceIdType.MESH
F32 = jnp.float32
BF16 = jnp.bfloat16


def dft_matrix(seg):
    phase = np.outer(4 * np.arange(seg) + 1, np.arange(seg)) % (4 * seg)
    angle = phase * (math.pi / (2 * seg))
    return np.concatenate([np.cos(angle), -np.sin(angle)], axis=0)


def halves(matrix):
    high = np.asarray(matrix, np.float32).astype(BF16)
    low = np.asarray(matrix - high.astype(np.float64), np.float32).astype(BF16)
    return high, low


def split(value):
    high = value.astype(BF16)
    return high, (value - high.astype(F32)).astype(BF16)


def mul_conj(a, b):
    return a[0] * b[0] + a[1] * b[1], a[1] * b[0] - a[0] * b[1]


def mul(a, b):
    return a[0] * b[0] - a[1] * b[1], a[0] * b[1] + a[1] * b[0]


def add(a, b):
    return a[0] + b[0], a[1] + b[1]


def turn(a):
    return -a[1], a[0]


def back(a):
    return a[1], -a[0]


def local_products(hs, ts):
    us = [None] + [add(ts[a], turn(ts[a - 1])) for a in range(1, len(ts))]
    first = mul_conj(hs[0], ts[0])
    for a in range(1, len(hs)):
        first = add(first, mul_conj(hs[a], us[a]))
    second = mul_conj(hs[1], ts[0])
    for a in range(2, len(hs)):
        second = add(second, mul_conj(hs[a], us[a - 1]))
    return first, second


def halo_products(first, second, h0, h1, t_near, t_before, h_after):
    one = mul_conj(h0, t_before)
    two = add(mul_conj(h1, t_before), mul_conj(h_after, t_near))
    return add(first, back(one)), add(add(second, one), back(two))


def own_products(f0, f1, s0, s1):
    first = mul(f0, s0)
    return first, add(turn(first), add(mul(f0, s1), mul(f1, s0)))


def plain_body(history, taps, self_taps, fresh, gate):
    n = lax.axis_size(AXIS)
    seg = fresh.shape[1] // 2
    matrix = jnp.asarray(dft_matrix(seg).astype(np.float32))
    hp = lax.Precision.HIGHEST
    before = lax.ppermute(taps[-seg:], AXIS, [(s, s + 1) for s in range(n - 1)])
    after = lax.ppermute(history[:seg], AXIS, [(s, s - 1) for s in range(1, n)])

    def forward(rows):
        spec = jnp.dot(matrix, rows, precision=hp)
        return spec[:seg], spec[seg:]

    def inverse(spec):
        return jnp.dot(matrix.T / seg, jnp.concatenate(spec, axis=0), precision=hp)

    count = history.shape[0] // seg
    hs = [forward(history[a * seg : (a + 1) * seg]) for a in range(count)]
    ts = [forward(taps[a * seg : (a + 1) * seg]) for a in range(count)]
    first, second = local_products(hs, ts)
    first, second = halo_products(first, second, hs[0], hs[1], ts[-2], forward(before), forward(after))
    part = jnp.concatenate([inverse(first), inverse(second)], axis=0).T
    summed = lax.psum_scatter(part, AXIS, scatter_dimension=0, tiled=True)
    f, s = fresh.T, self_taps.T
    own = own_products(forward(f[:seg]), forward(f[seg:]), forward(s[:seg]), forward(s[seg:]))
    own_part = jnp.concatenate([inverse(own[0]), inverse(own[1])], axis=0).T
    return gate * (summed + own_part)


def kernel(n, seg, hist, taps, self_taps_h, fresh_h, gate_h, fh_h, fl_h, gh_h, gl_h, out,
           self_taps, fresh, gate, fh, fl, gh, gl, hist_v, taps_v, tb, ha, sh0, sh1, st1, q0, q1, parts, d_recv, sums, y_send, y_recv, w_send, w_recv,
           p_recv, z_send, z_recv, x_send, x_recv, f_recv,
           small_sem, load_sem, tb_s, tb_r, ha_s, ha_r, d_s, d_r, y_s, y_r, w_s, w_r,
           p_s, p_r, z_s, z_r, x_s, x_r, f_s, f_r):
    me = lax.axis_index(AXIS)
    nz = n // PLANE
    my_z, low = me // PLANE, me % PLANE
    core, x, y = me % 2, low // 2 % 2, low // 4
    rows = hist.shape[0]
    count = rows // seg
    width = hist.shape[1] // nz
    block = width // PLANE
    partner = me + 1 - 2 * core
    routed = nz - DIRECT
    last = nz - 1
    half = width // 2
    x_peer, y_peer = me + 2 - 4 * x, me + 4 - 8 * y
    diagonal = me + 2 - 4 * x + 4 - 8 * y
    near = (y_peer, diagonal, x_peer)

    def pieces(i, dev):
        base = ((dev // PLANE + 1 + i) % nz) * width
        if i < last:
            return [(pl.ds(pl.multiple_of(base, width), width), pl.ds(0, width))]
        row = dev % PLANE // 4
        return [
            (pl.ds(pl.multiple_of(base + ((row + 1 + h) % 2) * half, half), half), pl.ds(h * half, half))
            for h in range(2)
        ]

    def remote(src, dst, send, recv, dev):
        return pltpu.make_async_remote_copy(
            src_ref=src, dst_ref=dst, send_sem=send, recv_sem=recv, device_id=(dev,), device_id_type=MESH
        )

    has_next, has_prev = me < n - 1, me > 0
    outer = me + 2 * core - 1
    has_outer = (outer >= 0) & (outer < n)
    peers = [partner]
    peers += near
    peers += [(dev + n - last * PLANE) % n for dev in near]
    peers += [(me + k * PLANE) % n for k in range(1, nz)]
    barrier = pltpu.get_barrier_semaphore()
    @pl.when(has_outer)
    def _():
        pl.semaphore_signal(barrier, inc=1, device_id=(outer,), device_id_type=MESH)

    for peer in peers:
        pl.semaphore_signal(barrier, inc=1, device_id=(peer,), device_id_type=MESH)

    small = [
        pltpu.make_async_copy(src, dst, small_sem.at[k])
        for k, (src, dst) in enumerate((
            (fh_h, fh), (fl_h, fl), (gh_h, gh), (gl_h, gl), (self_taps_h, self_taps), (fresh_h, fresh), (gate_h, gate),
        ))
    ]
    for copy in small:
        copy.start()
    loads = [[] for _ in range(nz)]
    for i in range(nz):
        for k, (src, dst) in enumerate(((hist, hist_v), (taps, taps_v))):
            for h, (here, there) in enumerate(pieces(i, me)):
                copy = pltpu.make_async_copy(src.at[:, here], dst.at[i, :, there], load_sem.at[k, i + h])
                copy.start()
                loads[i].append(copy)

    pl.semaphore_wait(barrier, len(peers) + jnp.where(has_outer, 1, 0))

    def taps_copies(i, dev):
        return [
            remote(taps.at[pl.ds(rows - seg, seg), here], tb.at[i, :, there], tb_s.at[i + h], tb_r.at[i + h], dev)
            for h, (here, there) in enumerate(pieces(i, dev))
        ]

    def hist_copies(i, dev):
        return [
            remote(hist.at[pl.ds(0, seg), here], ha.at[i, :, there], ha_s.at[i + h], ha_r.at[i + h], dev)
            for h, (here, there) in enumerate(pieces(i, dev))
        ]

    def send_halo(i):
        @pl.when(has_next)
        def _():
            for copy in taps_copies(i, me + 1):
                copy.start()

        @pl.when(has_prev)
        def _():
            for copy in hist_copies(i, me - 1):
                copy.start()

    for i in range(min(AHEAD, nz)):
        send_halo(i)

    def forward(value):
        both = jnp.concatenate(split(value), axis=0)
        spec = jnp.dot(fh[...], both, preferred_element_type=F32) + jnp.dot(
            fl[...], both, preferred_element_type=F32
        )
        return spec[:seg], spec[seg:]

    def keep(ref, i, spec):
        ref[i, :seg], ref[i, seg:] = spec

    def held(ref, i, at):
        return ref[i, :seg, at], ref[i, seg:, at]

    @pl.when(me == 0)
    def _():
        tb[...] = jnp.zeros_like(tb)

    @pl.when(me == n - 1)
    def _():
        ha[...] = jnp.zeros_like(ha)

    for copy in small:
        copy.wait()
    for i in range(nz):
        for copy in loads[i]:
            copy.wait()
        hs = [forward(hist_v[i, pl.ds(a * seg, seg)]) for a in range(count)]
        ts = [forward(taps_v[i, pl.ds(a * seg, seg)]) for a in range(count)]
        first, second = local_products(hs, ts)
        keep(sh0, i, hs[0])
        keep(sh1, i, hs[1])
        keep(st1, i, ts[-2])
        keep(q0, i, first)
        keep(q1, i, second)

    contract = (((1,), (1,)), ((), ()))

    def dot_t(a, b):
        return lax.dot_general(a, b, contract, preferred_element_type=F32)

    f, s = fresh[...], self_taps[...]
    both = jnp.concatenate(split(jnp.concatenate([f[:, :seg], f[:, seg:], s[:, :seg], s[:, seg:]], axis=0)), axis=1)
    spec = dot_t(both, fh[...]) + dot_t(both, fl[...])
    quads = [(spec[k * block : (k + 1) * block, :seg], spec[k * block : (k + 1) * block, seg:]) for k in range(4)]
    a, b = own_products(*quads)
    high, low_half = split(jnp.concatenate([jnp.concatenate(a, axis=1), jnp.concatenate(b, axis=1)], axis=0))
    res = dot_t(high, gh[...]) + dot_t(low_half, gh[...]) + dot_t(high, gl[...])
    own = jnp.concatenate([res[:block], res[block:]], axis=1)

    def inverse(spec):
        hi, lo = split(jnp.concatenate(spec, axis=0))
        return (
            jnp.dot(gh[...], hi, preferred_element_type=F32)
            + jnp.dot(gh[...], lo, preferred_element_type=F32)
            + jnp.dot(gl[...], hi, preferred_element_type=F32)
        ).T

    def chip_copy(i, h=None):
        span, k = (pl.ds(0, 4), i) if h is None else (pl.ds(2 * h, 2), i + h)
        return remote(parts.at[i, 1 - core, span], d_recv.at[i, span], d_s.at[k], d_r.at[k], partner)

    def y_copy(i):
        return remote(y_send.at[i], y_recv.at[i], y_s.at[i], y_r.at[i], y_peer)

    def w_copy(i):
        return remote(w_send.at[i], w_recv.at[i], w_s.at[i], w_r.at[i], (me + (i + 1) * PLANE) % n)

    def near_copy(i, j):
        k = i - routed
        return remote(sums.at[k, (0, 1, 3)[j]], p_recv.at[k, j], p_s.at[k, j], p_r.at[k, j], near[j])

    def z_copy(i):
        k = i - routed
        return remote(z_send.at[k], z_recv.at[k], z_s.at[k], z_r.at[k], (me + (i + 1) * PLANE) % n)

    def x_copy():
        return remote(x_send, x_recv, x_s, x_r, x_peer)

    def far_copy(place):
        dev = ((y_peer, diagonal, me, x_peer)[place] + last * PLANE) % n
        return remote(sums.at[last - 1 - routed, place], f_recv.at[place], f_s.at[place], f_r.at[place], dev)

    def compute(i, h=None):
        which = slice(None) if h is None else slice(h, h + 1)

        @pl.when(has_prev)
        def _():
            for copy in taps_copies(i, me)[which]:
                copy.wait_recv()

        @pl.when(has_next)
        def _():
            for copy in hist_copies(i, me)[which]:
                copy.wait_recv()

        at = pl.ds(0, width) if h is None else pl.ds(h * half, half)
        both = halo_products(
            held(q0, i, at), held(q1, i, at), held(sh0, i, at), held(sh1, i, at), held(st1, i, at),
            forward(tb[i, :, at]), forward(ha[i, :, at]),
        )
        for side, spec in enumerate(both):
            res = inverse(spec)
            for k in range(res.shape[0] // block):
                col = k // 2 % 2
                row = (k // 4 + y + 1) % 2 if h is None else h
                place = 2 * row + (col + x) % 2
                parts[i, k % 2, place, :, pl.ds(side * seg, seg)] = res[k * block : (k + 1) * block]
        chip_copy(i, h).start()

    def route_y(i):
        chip_copy(i).wait_recv()
        y_send[i] = parts[i, core, :2] + d_recv[i, :2]
        y_copy(i).start()

    def route_z(i):
        y_copy(i).wait_recv()
        w_send[i] = parts[i, core, 2:] + d_recv[i, 2:] + y_recv[i]
        w_copy(i).start()

    def spread(i, h=None):
        chip_copy(i, h).wait_recv()
        lo, hi = (0, 4) if h is None else (2 * h, 2 * h + 2)
        sums[i - routed, lo:hi] = parts[i, core, lo:hi] + d_recv[i, lo:hi]
        if i == last - 1:
            for place in range(4):
                far_copy(place).start()
            return
        for j, place in enumerate((0, 1, 3)):
            if lo <= place < hi:
                near_copy(i, j).start()

    def gathered(i):
        for j in range(3):
            near_copy(i, j).wait_recv()
        k = i - routed
        return sums[k, 2] + p_recv[k, 0] + p_recv[k, 1] + p_recv[k, 2]

    for i in range(last):
        compute(i)
        if i < routed:
            route_y(i)
        else:
            spread(i)
        if i + AHEAD < nz:
            send_halo(i + AHEAD)
        if 0 <= i - 1 < routed:
            route_z(i - 1)
    compute(last, 0)
    if routed == last:
        route_z(last - 1)
    spread(last, 0)
    compute(last, 1)
    spread(last, 1)
    for i in range(routed, last - 1):
        z_send[i - routed] = gathered(i)
        z_copy(i).start()
    for i in range(routed):
        w_copy(i).wait_recv()
    total = gathered(last)
    if routed:
        merged = w_recv[0]
        for i in range(1, routed):
            merged = merged + w_recv[i]
        x_send[...] = merged[1]
        x_copy().start()
        total = total + merged[0]
    for i in range(routed, last - 1):
        z_copy(i).wait_recv()
        total = total + z_recv[i - routed]
    for place in range(4):
        far_copy(place).wait_recv()
        total = total + f_recv[place]
    if routed:
        x_copy().wait_recv()
        total = total + x_recv[...]
        x_copy().wait_send()
    out[...] = gate[...] * (total + own)

    for i in range(nz):
        @pl.when(has_next)
        def _(i=i):
            for copy in taps_copies(i, me + 1):
                copy.wait_send()

        @pl.when(has_prev)
        def _(i=i):
            for copy in hist_copies(i, me - 1):
                copy.wait_send()

        for h in (None,) if i < last else (0, 1):
            chip_copy(i, h).wait_send()
        if i < routed:
            y_copy(i).wait_send()
            w_copy(i).wait_send()
        elif i == last - 1:
            for place in range(4):
                far_copy(place).wait_send()
        else:
            for j in range(3):
                near_copy(i, j).wait_send()
            if i < last - 1:
                z_copy(i).wait_send()


def kernel_body(history, taps, self_taps, fresh, gate):
    n = lax.axis_size(AXIS)
    rows, channels = history.shape
    block, new_len = fresh.shape
    seg = new_len // 2
    nz = n // PLANE
    width = channels // nz
    fh, fl = halves(dft_matrix(seg))
    gh, gl = halves(dft_matrix(seg).T / seg)
    fh, fl = np.concatenate([fh, fh], axis=1), np.concatenate([fl, fl], axis=1)
    vmem = pl.BlockSpec(memory_space=pltpu.VMEM)
    hbm = pl.BlockSpec(memory_space=pl.ANY)
    chips = PLANE // 2
    dma = pltpu.SemaphoreType.DMA
    spec = pltpu.VMEM((nz, 2 * seg, width), F32)
    pair = pltpu.VMEM((max(nz - DIRECT, 1), 2, block, new_len), F32)
    return pl.pallas_call(
        lambda *refs: kernel(n, seg, *refs),
        out_shape=pltpu.VMEM(fresh.shape, F32),
        in_specs=[hbm] * 9,
        out_specs=vmem,
        scratch_shapes=[
            pltpu.VMEM(fresh.shape, F32), pltpu.VMEM(fresh.shape, F32), pltpu.VMEM(fresh.shape, F32),
            pltpu.VMEM(fh.shape, BF16), pltpu.VMEM(fh.shape, BF16), pltpu.VMEM(gh.shape, BF16), pltpu.VMEM(gh.shape, BF16),
            pltpu.VMEM((nz, rows, width), F32),
            pltpu.VMEM((nz, rows, width), F32),
            pltpu.VMEM((nz, seg, width), F32),
            pltpu.VMEM((nz, seg, width), F32),
            spec, spec, spec, spec, spec,
            pltpu.VMEM((nz, 2, chips, block, new_len), F32),
            pltpu.VMEM((nz, chips, block, new_len), F32),
            pltpu.VMEM((DIRECT, chips, block, new_len), F32),
            pair, pair, pair, pair,
            pltpu.VMEM((DIRECT, 3, block, new_len), F32),
            pltpu.VMEM((DIRECT, block, new_len), F32),
            pltpu.VMEM((DIRECT, block, new_len), F32),
            pltpu.VMEM((block, new_len), F32),
            pltpu.VMEM((block, new_len), F32),
            pltpu.VMEM((4, block, new_len), F32),
            dma((7,)),
            dma((2, nz + 1)),
            dma((nz + 1,)), dma((nz + 1,)), dma((nz + 1,)), dma((nz + 1,)),
            dma((nz + 1,)), dma((nz + 1,)),
            dma((nz,)), dma((nz,)), dma((nz,)), dma((nz,)),
            dma((DIRECT, 3)), dma((DIRECT, 3)),
            dma((DIRECT,)), dma((DIRECT,)),
            dma, dma,
            dma((4,)), dma((4,)),
        ],
        compiler_params=pltpu.CompilerParams(collective_id=0, has_side_effects=True),
        name="hyena",
    )(history, taps, self_taps, fresh, gate, *(jnp.asarray(m) for m in (fh, fl, gh, gl)))


def solution(mesh):
    n = mesh.shape[AXIS]

    def body(history, taps, self_taps, fresh, gate):
        channels = history.shape[1]
        block = fresh.shape[0]
        fits = n % PLANE == 0 and n >= DIRECT * PLANE and block % 8 == 0 and (block * PLANE) % 256 == 0
        chosen = kernel_body if fits and channels == block * n else plain_body
        return chosen(history, taps, self_taps, fresh, gate)

    spec = P(AXIS, None)
    return jax.shard_map(body, mesh=mesh, in_specs=(spec,) * 5, out_specs=spec, check_vma=False)
```

```python
import math

import jax
import jax.numpy as jnp
import numpy as np
from jax import lax
from jax.experimental import pallas as pl
from jax.experimental.pallas import tpu as pltpu
from jax.sharding import PartitionSpec as P

AXIS = "seq"
AHEAD = 3
DIRECT = 3
PLANE = 8
MESH = pl.DeviceIdType.MESH
F32 = jnp.float32
BF16 = jnp.bfloat16


def dft_matrix(seg):
    phase = np.outer(4 * np.arange(seg) + 1, np.arange(seg)) % (4 * seg)
    angle = phase * (math.pi / (2 * seg))
    return np.concatenate([np.cos(angle), -np.sin(angle)], axis=0)


def halves(matrix):
    high = np.asarray(matrix, np.float32).astype(BF16)
    low = np.asarray(matrix - high.astype(np.float64), np.float32).astype(BF16)
    return high, low


def split(value):
    high = value.astype(BF16)
    return high, (value - high.astype(F32)).astype(BF16)


def mul_conj(a, b):
    return a[0] * b[0] + a[1] * b[1], a[1] * b[0] - a[0] * b[1]


def mul(a, b):
    return a[0] * b[0] - a[1] * b[1], a[0] * b[1] + a[1] * b[0]


def add(a, b):
    return a[0] + b[0], a[1] + b[1]


def turn(a):
    return -a[1], a[0]


def back(a):
    return a[1], -a[0]


def local_products(hs, ts):
    us = [None] + [add(ts[a], turn(ts[a - 1])) for a in range(1, len(ts))]
    first = mul_conj(hs[0], ts[0])
    for a in range(1, len(hs)):
        first = add(first, mul_conj(hs[a], us[a]))
    second = mul_conj(hs[1], ts[0])
    for a in range(2, len(hs)):
        second = add(second, mul_conj(hs[a], us[a - 1]))
    return first, second


def halo_products(first, second, h0, h1, t_near, t_before, h_after):
    one = mul_conj(h0, t_before)
    two = add(mul_conj(h1, t_before), mul_conj(h_after, t_near))
    return add(first, back(one)), add(add(second, one), back(two))


def own_products(f0, f1, s0, s1):
    first = mul(f0, s0)
    return first, add(turn(first), add(mul(f0, s1), mul(f1, s0)))


def plain_body(history, taps, self_taps, fresh, gate):
    n = lax.axis_size(AXIS)
    seg = fresh.shape[1] // 2
    matrix = jnp.asarray(dft_matrix(seg).astype(np.float32))
    hp = lax.Precision.HIGHEST
    before = lax.ppermute(taps[-seg:], AXIS, [(s, s + 1) for s in range(n - 1)])
    after = lax.ppermute(history[:seg], AXIS, [(s, s - 1) for s in range(1, n)])

    def forward(rows):
        spec = jnp.dot(matrix, rows, precision=hp)
        return spec[:seg], spec[seg:]

    def inverse(spec):
        return jnp.dot(matrix.T / seg, jnp.concatenate(spec, axis=0), precision=hp)

    count = history.shape[0] // seg
    hs = [forward(history[a * seg : (a + 1) * seg]) for a in range(count)]
    ts = [forward(taps[a * seg : (a + 1) * seg]) for a in range(count)]
    first, second = local_products(hs, ts)
    first, second = halo_products(first, second, hs[0], hs[1], ts[-2], forward(before), forward(after))
    part = jnp.concatenate([inverse(first), inverse(second)], axis=0).T
    summed = lax.psum_scatter(part, AXIS, scatter_dimension=0, tiled=True)
    f, s = fresh.T, self_taps.T
    own = own_products(forward(f[:seg]), forward(f[seg:]), forward(s[:seg]), forward(s[seg:]))
    own_part = jnp.concatenate([inverse(own[0]), inverse(own[1])], axis=0).T
    return gate * (summed + own_part)


def kernel(n, seg, hist, taps, self_taps_h, fresh_h, gate_h, fh_h, fl_h, gh_h, gl_h, out,
           self_taps, fresh, gate, fh, fl, gh, gl, hist_v, taps_v, tb, ha, sh0, sh1, st1, q0, q1, parts, d_recv, sums, y_send, y_recv, w_send, w_recv,
           p_recv, z_send, z_recv, x_send, x_recv,
           small_sem, load_sem, tb_s, tb_r, ha_s, ha_r, d_s, d_r, y_s, y_r, w_s, w_r,
           p_s, p_r, z_s, z_r, x_s, x_r):
    me = lax.axis_index(AXIS)
    nz = n // PLANE
    my_z, low = me // PLANE, me % PLANE
    core, x, y = me % 2, low // 2 % 2, low // 4
    rows = hist.shape[0]
    count = rows // seg
    width = hist.shape[1] // nz
    block = width // PLANE
    partner = me + 1 - 2 * core
    routed = nz - DIRECT
    last = nz - 1
    half = width // 2
    x_peer, y_peer = me + 2 - 4 * x, me + 4 - 8 * y
    diagonal = me + 2 - 4 * x + 4 - 8 * y
    near = (y_peer, diagonal, x_peer)

    def pieces(i, dev):
        base = ((dev // PLANE + 1 + i) % nz) * width
        if i < last:
            return [(pl.ds(pl.multiple_of(base, width), width), pl.ds(0, width))]
        row = dev % PLANE // 4
        return [
            (pl.ds(pl.multiple_of(base + ((row + 1 + h) % 2) * half, half), half), pl.ds(h * half, half))
            for h in range(2)
        ]

    def remote(src, dst, send, recv, dev):
        return pltpu.make_async_remote_copy(
            src_ref=src, dst_ref=dst, send_sem=send, recv_sem=recv, device_id=(dev,), device_id_type=MESH
        )

    has_next, has_prev = me < n - 1, me > 0
    outer = me + 2 * core - 1
    has_outer = (outer >= 0) & (outer < n)
    peers = [partner]
    peers += near
    peers += [(me + k * PLANE) % n for k in range(1, nz)]
    barrier = pltpu.get_barrier_semaphore()
    @pl.when(has_outer)
    def _():
        pl.semaphore_signal(barrier, inc=1, device_id=(outer,), device_id_type=MESH)

    for peer in peers:
        pl.semaphore_signal(barrier, inc=1, device_id=(peer,), device_id_type=MESH)

    small = [
        pltpu.make_async_copy(src, dst, small_sem.at[k])
        for k, (src, dst) in enumerate((
            (fh_h, fh), (fl_h, fl), (gh_h, gh), (gl_h, gl), (self_taps_h, self_taps), (fresh_h, fresh), (gate_h, gate),
        ))
    ]
    for copy in small:
        copy.start()
    loads = [[] for _ in range(nz)]
    for i in range(nz):
        for k, (src, dst) in enumerate(((hist, hist_v), (taps, taps_v))):
            for h, (here, there) in enumerate(pieces(i, me)):
                copy = pltpu.make_async_copy(src.at[:, here], dst.at[i, :, there], load_sem.at[k, i + h])
                copy.start()
                loads[i].append(copy)

    pl.semaphore_wait(barrier, len(peers) + jnp.where(has_outer, 1, 0))

    def taps_copies(i, dev):
        return [
            remote(taps.at[pl.ds(rows - seg, seg), here], tb.at[i, :, there], tb_s.at[i + h], tb_r.at[i + h], dev)
            for h, (here, there) in enumerate(pieces(i, dev))
        ]

    def hist_copies(i, dev):
        return [
            remote(hist.at[pl.ds(0, seg), here], ha.at[i, :, there], ha_s.at[i + h], ha_r.at[i + h], dev)
            for h, (here, there) in enumerate(pieces(i, dev))
        ]

    def send_halo(i):
        @pl.when(has_next)
        def _():
            for copy in taps_copies(i, me + 1):
                copy.start()

        @pl.when(has_prev)
        def _():
            for copy in hist_copies(i, me - 1):
                copy.start()

    for i in range(min(AHEAD, nz)):
        send_halo(i)

    def forward(value):
        both = jnp.concatenate(split(value), axis=0)
        spec = jnp.dot(fh[...], both, preferred_element_type=F32) + jnp.dot(
            fl[...], both, preferred_element_type=F32
        )
        return spec[:seg], spec[seg:]

    def keep(ref, i, spec):
        ref[i, :seg], ref[i, seg:] = spec

    def held(ref, i, at):
        return ref[i, :seg, at], ref[i, seg:, at]

    @pl.when(me == 0)
    def _():
        tb[...] = jnp.zeros_like(tb)

    @pl.when(me == n - 1)
    def _():
        ha[...] = jnp.zeros_like(ha)

    for copy in small:
        copy.wait()
    for i in range(nz):
        for copy in loads[i]:
            copy.wait()
        hs = [forward(hist_v[i, pl.ds(a * seg, seg)]) for a in range(count)]
        ts = [forward(taps_v[i, pl.ds(a * seg, seg)]) for a in range(count)]
        first, second = local_products(hs, ts)
        keep(sh0, i, hs[0])
        keep(sh1, i, hs[1])
        keep(st1, i, ts[-2])
        keep(q0, i, first)
        keep(q1, i, second)

    contract = (((1,), (1,)), ((), ()))

    def dot_t(a, b):
        return lax.dot_general(a, b, contract, preferred_element_type=F32)

    f, s = fresh[...], self_taps[...]
    both = jnp.concatenate(split(jnp.concatenate([f[:, :seg], f[:, seg:], s[:, :seg], s[:, seg:]], axis=0)), axis=1)
    spec = dot_t(both, fh[...]) + dot_t(both, fl[...])
    quads = [(spec[k * block : (k + 1) * block, :seg], spec[k * block : (k + 1) * block, seg:]) for k in range(4)]
    a, b = own_products(*quads)
    high, low_half = split(jnp.concatenate([jnp.concatenate(a, axis=1), jnp.concatenate(b, axis=1)], axis=0))
    res = dot_t(high, gh[...]) + dot_t(low_half, gh[...]) + dot_t(high, gl[...])
    own = jnp.concatenate([res[:block], res[block:]], axis=1)

    def inverse(spec):
        hi, lo = split(jnp.concatenate(spec, axis=0))
        return (
            jnp.dot(gh[...], hi, preferred_element_type=F32)
            + jnp.dot(gh[...], lo, preferred_element_type=F32)
            + jnp.dot(gl[...], hi, preferred_element_type=F32)
        ).T

    def chip_copy(i, h=None):
        span, k = (pl.ds(0, 4), i) if h is None else (pl.ds(2 * h, 2), i + h)
        return remote(parts.at[i, 1 - core, span], d_recv.at[i, span], d_s.at[k], d_r.at[k], partner)

    def y_copy(i):
        return remote(y_send.at[i], y_recv.at[i], y_s.at[i], y_r.at[i], y_peer)

    def w_copy(i):
        return remote(w_send.at[i], w_recv.at[i], w_s.at[i], w_r.at[i], (me + (i + 1) * PLANE) % n)

    def near_copy(i, j):
        k = i - routed
        return remote(sums.at[k, (0, 1, 3)[j]], p_recv.at[k, j], p_s.at[k, j], p_r.at[k, j], near[j])

    def z_copy(i):
        k = i - routed
        return remote(z_send.at[k], z_recv.at[k], z_s.at[k], z_r.at[k], (me + (i + 1) * PLANE) % n)

    def x_copy():
        return remote(x_send, x_recv, x_s, x_r, x_peer)

    def compute(i, h=None):
        which = slice(None) if h is None else slice(h, h + 1)

        @pl.when(has_prev)
        def _():
            for copy in taps_copies(i, me)[which]:
                copy.wait_recv()

        @pl.when(has_next)
        def _():
            for copy in hist_copies(i, me)[which]:
                copy.wait_recv()

        at = pl.ds(0, width) if h is None else pl.ds(h * half, half)
        both = halo_products(
            held(q0, i, at), held(q1, i, at), held(sh0, i, at), held(sh1, i, at), held(st1, i, at),
            forward(tb[i, :, at]), forward(ha[i, :, at]),
        )
        for side, spec in enumerate(both):
            res = inverse(spec)
            for k in range(res.shape[0] // block):
                col = k // 2 % 2
                row = (k // 4 + y + 1) % 2 if h is None else h
                place = 2 * row + (col + x) % 2
                parts[i, k % 2, place, :, pl.ds(side * seg, seg)] = res[k * block : (k + 1) * block]
        chip_copy(i, h).start()

    def route_y(i):
        chip_copy(i).wait_recv()
        y_send[i] = parts[i, core, :2] + d_recv[i, :2]
        y_copy(i).start()

    def route_z(i):
        y_copy(i).wait_recv()
        w_send[i] = parts[i, core, 2:] + d_recv[i, 2:] + y_recv[i]
        w_copy(i).start()

    def spread(i, h=None):
        chip_copy(i, h).wait_recv()
        lo, hi = (0, 4) if h is None else (2 * h, 2 * h + 2)
        sums[i - routed, lo:hi] = parts[i, core, lo:hi] + d_recv[i, lo:hi]
        for j, place in enumerate((0, 1, 3)):
            if lo <= place < hi:
                near_copy(i, j).start()

    def gathered(i):
        for j in range(3):
            near_copy(i, j).wait_recv()
        k = i - routed
        return sums[k, 2] + p_recv[k, 0] + p_recv[k, 1] + p_recv[k, 2]

    def send_z(i):
        z_send[i - routed] = gathered(i)
        z_copy(i).start()

    for i in range(last):
        compute(i)
        if i < routed:
            route_y(i)
        else:
            spread(i)
        if i + AHEAD < nz:
            send_halo(i + AHEAD)
        if 0 <= i - 1 < routed:
            route_z(i - 1)
        elif i - 1 >= routed:
            send_z(i - 1)
    compute(last, 0)
    if routed == last:
        route_z(last - 1)
    spread(last, 0)
    compute(last, 1)
    spread(last, 1)
    if routed < last:
        send_z(last - 1)
    for i in range(routed):
        w_copy(i).wait_recv()
    total = gathered(last)
    if routed:
        merged = w_recv[0]
        for i in range(1, routed):
            merged = merged + w_recv[i]
        x_send[...] = merged[1]
        x_copy().start()
        total = total + merged[0]
    for i in range(routed, last):
        z_copy(i).wait_recv()
        total = total + z_recv[i - routed]
    if routed:
        x_copy().wait_recv()
        total = total + x_recv[...]
        x_copy().wait_send()
    out[...] = gate[...] * (total + own)

    for i in range(nz):
        @pl.when(has_next)
        def _(i=i):
            for copy in taps_copies(i, me + 1):
                copy.wait_send()

        @pl.when(has_prev)
        def _(i=i):
            for copy in hist_copies(i, me - 1):
                copy.wait_send()

        for h in (None,) if i < last else (0, 1):
            chip_copy(i, h).wait_send()
        if i < routed:
            y_copy(i).wait_send()
            w_copy(i).wait_send()
        else:
            for j in range(3):
                near_copy(i, j).wait_send()
            if i < last:
                z_copy(i).wait_send()


def kernel_body(history, taps, self_taps, fresh, gate):
    n = lax.axis_size(AXIS)
    rows, channels = history.shape
    block, new_len = fresh.shape
    seg = new_len // 2
    nz = n // PLANE
    width = channels // nz
    fh, fl = halves(dft_matrix(seg))
    gh, gl = halves(dft_matrix(seg).T / seg)
    fh, fl = np.concatenate([fh, fh], axis=1), np.concatenate([fl, fl], axis=1)
    vmem = pl.BlockSpec(memory_space=pltpu.VMEM)
    hbm = pl.BlockSpec(memory_space=pl.ANY)
    chips = PLANE // 2
    dma = pltpu.SemaphoreType.DMA
    spec = pltpu.VMEM((nz, 2 * seg, width), F32)
    pair = pltpu.VMEM((max(nz - DIRECT, 1), 2, block, new_len), F32)
    return pl.pallas_call(
        lambda *refs: kernel(n, seg, *refs),
        out_shape=pltpu.VMEM(fresh.shape, F32),
        in_specs=[hbm] * 9,
        out_specs=vmem,
        scratch_shapes=[
            pltpu.VMEM(fresh.shape, F32), pltpu.VMEM(fresh.shape, F32), pltpu.VMEM(fresh.shape, F32),
            pltpu.VMEM(fh.shape, BF16), pltpu.VMEM(fh.shape, BF16), pltpu.VMEM(gh.shape, BF16), pltpu.VMEM(gh.shape, BF16),
            pltpu.VMEM((nz, rows, width), F32),
            pltpu.VMEM((nz, rows, width), F32),
            pltpu.VMEM((nz, seg, width), F32),
            pltpu.VMEM((nz, seg, width), F32),
            spec, spec, spec, spec, spec,
            pltpu.VMEM((nz, 2, chips, block, new_len), F32),
            pltpu.VMEM((nz, chips, block, new_len), F32),
            pltpu.VMEM((DIRECT, chips, block, new_len), F32),
            pair, pair, pair, pair,
            pltpu.VMEM((DIRECT, 3, block, new_len), F32),
            pltpu.VMEM((DIRECT, block, new_len), F32),
            pltpu.VMEM((DIRECT, block, new_len), F32),
            pltpu.VMEM((block, new_len), F32),
            pltpu.VMEM((block, new_len), F32),
            dma((7,)),
            dma((2, nz + 1)),
            dma((nz + 1,)), dma((nz + 1,)), dma((nz + 1,)), dma((nz + 1,)),
            dma((nz + 1,)), dma((nz + 1,)),
            dma((nz,)), dma((nz,)), dma((nz,)), dma((nz,)),
            dma((DIRECT, 3)), dma((DIRECT, 3)),
            dma((DIRECT,)), dma((DIRECT,)),
            dma, dma,
        ],
        compiler_params=pltpu.CompilerParams(collective_id=0, has_side_effects=True),
        name="hyena",
    )(history, taps, self_taps, fresh, gate, *(jnp.asarray(m) for m in (fh, fl, gh, gl)))


def solution(mesh):
    n = mesh.shape[AXIS]

    def body(history, taps, self_taps, fresh, gate):
        channels = history.shape[1]
        block = fresh.shape[0]
        fits = n % PLANE == 0 and n >= DIRECT * PLANE and block % 8 == 0 and (block * PLANE) % 256 == 0
        chosen = kernel_body if fits and channels == block * n else plain_body
        return chosen(history, taps, self_taps, fresh, gate)

    spec = P(AXIS, None)
    return jax.shard_map(body, mesh=mesh, in_specs=(spec,) * 5, out_specs=spec, check_vma=False)
```
